256 devices in a mesh: groups: 2 (over y), seq: 64 (over x, z), section: 2 (over core).
Axes of the slice: x: 4, y: 2, z: 16, core: 2. Of those that a mesh axis runs over, the one named last changes fastest.
The devices are a block of a 4x16x16 slice.
Arguments:
- hidden_in: bfloat16 [4, 8192], P('groups', 'seq'), parts along dimension 0, may hold values from -40 to 40
- norm_gain: bfloat16 [2, 8192], P('section', 'seq'), may hold values from 0.5 to 1.5
- qkv_weight: bfloat16 [2, 8192, 10240], P('section', 'seq'), as said below
- out_weight: bfloat16 [2, 8192, 8192], P('section', None, 'seq'), may hold values from -0.0625 to 0.0625
- memory: bfloat16 [2, 4, 8, 256, 2, 128, 128], P('section', 'groups', None, 'seq'), parts along dimension 1, may hold values from -12 to 12
- lengths: int32 [4], P('groups'), parts along dimension 0, may hold values from 16384 to 32768
- selected: int32 [4, 8, 16], P('groups'), parts along dimension 0, may hold values from 0 to 255, all different within a row
Outputs:
- hidden_out: bfloat16 [2, 4, 8192], P('section', 'groups', 'seq'), parts along dimension 1
- attention: bfloat16 [2, 4, 8192], P('section', 'groups'), parts along dimension 1
The draws below stay inside these ranges and needn't reach their ends.
There are 2 independent parts, one for each index of `groups`. The reference program is written for one: setup_inputs(seed, part) draws one part's arguments, and reference() takes and returns one part's arrays. A program takes and returns all parts, laid end to end along the dimension named above; an argument that names none is the same for every part. Nothing has to cross between parts.
Inputs may be any that keep to these rules, and one draw needn't show every extreme that they name: `selected`: for each sequence and key-value head the 16 block numbers differ. `qkv_weight`: every entry's magnitude is at most 256 / sqrt(8192).
All inputs are finite; a program needn't handle non-finite values.
Results may differ from the reference program's by a relative error of at most 0.025.
The reference program's roundings to bfloat16 on the way count: a program that leaves them out, or rounds other values in their place, can miss the bound.
Values may be sent and summed in bfloat16 or wider, within the bound.
A program may use at most 128 MiB of HBM per device.

```python
import jax
import jax.numpy as jnp
from jax import lax

D = 8192
HEADS = 64
KVH = 8
HEAD = 128
BLOCK = 128
SEL = 16
SEQS = 2
NBLK = 256
LAYERS = 2
QKVW = 10240


def draw_qkv_weight(key, part):
    base_draw = jax.random.normal(key, (LAYERS, D, QKVW), jnp.float32)
    base_draw = jnp.clip(base_draw, -4.0, 4.0) * D ** (-0.5)
    return base_draw.astype(jnp.bfloat16)


def draw_hidden_in(key, part):
    column_pos = jnp.arange(D, dtype=jnp.float32) / max(D - 1, 1)
    base_draw = jnp.clip(jax.random.normal(key, (SEQS, D), jnp.float32), -5.0, 5.0)
    column_scale = jnp.exp(jnp.log(4.0) * column_pos)
    base_draw = base_draw * column_scale[None, :] * 0.5
    return jnp.clip(base_draw, -40.0, 40.0).astype(jnp.bfloat16)


def level_of(stream_key, dims, shards, low, top_value):
    def one(axis_at, parts):
        heights = jax.random.uniform(jax.random.fold_in(jax.random.fold_in(stream_key, 6), axis_at), (parts,), jnp.float32, low / len(shards), top_value / len(shards))
        return jnp.repeat(jnp.exp(heights), dims[axis_at] // parts).reshape((-1,) + (1,) * (len(dims) - axis_at - 1))

    factor_of = one(*shards[0])
    for cut in shards[1:]:
        factor_of = factor_of * one(*cut)
    return factor_of


def different_ones(own_key, rows, number_of, top, lift):
    order = jax.random.permutation(jax.random.fold_in(own_key, 1), number_of)
    favour = order
    for power in range(3):
        favour = favour * favour // number_of
    favour = favour * lift // number_of
    chance = jax.random.randint(jax.random.fold_in(own_key, 2), (rows, number_of), 0, 4096) + favour
    holders = jax.random.permutation(jax.random.fold_in(own_key, 3), rows)[jnp.arange(number_of) % rows]
    chance = jnp.where(jnp.arange(rows)[:, None] == holders[None, :], 1 << 14, chance)
    merit = chance * number_of + jnp.arange(number_of)
    return lax.top_k(merit.astype(jnp.int32), top)[1].astype(jnp.int32)


def gaussian(rng, dims, width, reach, pieces=(), held_as=jnp.bfloat16):
    entries = width * jax.random.normal(rng, dims, jnp.float32)
    if pieces:
        entries = entries * level_of(rng, dims, pieces, -0.22, 0.18)
    return jnp.clip(entries, -reach, reach).astype(held_as)


def setup_inputs(seed: int = 0, part: int = 0) -> dict:
    splits = jax.random.split(jax.random.key(seed), 8)
    part_splits = jax.random.split(jax.random.fold_in(splits[7], part), 8)
    hidden_in = draw_hidden_in(jax.random.fold_in(jax.random.fold_in(splits[7], part), 71), part)
    norm_gain = jnp.clip(1.0 + 0.1 * jax.random.normal(splits[1], (LAYERS, D), jnp.float32), 0.5, 1.5).astype(jnp.bfloat16)
    qkv_weight = draw_qkv_weight(jax.random.fold_in(splits[7], 71), part)
    out_weight = gaussian(splits[3], (LAYERS, HEADS * HEAD, D), (HEADS * HEAD) ** -0.5, 0.0625, ((0, 2), (2, 64)))
    memory = gaussian(part_splits[4], (LAYERS, SEQS, KVH, NBLK, 2, BLOCK, HEAD), 2.0, 12.0, ((0, 2), (3, 64)))
    lengths = jax.random.randint(part_splits[5], (SEQS,), NBLK * BLOCK // 2, NBLK * BLOCK + 1).astype(jnp.int32)
    selected = different_ones(part_splits[6], SEQS * KVH, NBLK, SEL, 1024).reshape((SEQS, KVH, SEL))
    return {"hidden_in": hidden_in, "norm_gain": norm_gain, "qkv_weight": qkv_weight, "out_weight": out_weight, "memory": memory, "lengths": lengths, "selected": selected}


EPSILON = 1e-05
FLOOR = -1e+30

def pick_blocks(layer_memory, chosen_ids):
    return jax.vmap(jax.vmap(lambda blocks, ids: blocks[ids]))(layer_memory, chosen_ids)

def reference(hidden_in, norm_gain, qkv_weight, out_weight, memory, lengths, selected):
    heads_total = HEADS * HEAD
    kv_width = KVH * HEAD
    group_size = HEADS // KVH
    score_scale = HEAD ** (-0.5)
    offsets = jnp.arange(BLOCK, dtype=jnp.int32)
    positions = (selected[..., None] * BLOCK + offsets).reshape(SEQS, KVH, SEL * BLOCK)
    live_mask = positions < lengths[:, None, None]
    current = hidden_in
    hidden_list = []
    attention_list = []
    for layer_index in range(LAYERS):
        hidden_wide = current.astype(jnp.float32)
        squares = lax.optimization_barrier(jnp.sum(hidden_wide * hidden_wide, axis=1))
        normed = (hidden_wide * norm_gain[layer_index].astype(jnp.float32)).astype(jnp.bfloat16)
        summed = jnp.dot(normed, qkv_weight[layer_index], preferred_element_type=jnp.float32)
        projected = (summed * lax.rsqrt(squares / D + EPSILON)[:, None]).astype(jnp.bfloat16)
        queries = projected[:, :heads_total].reshape(SEQS, KVH, group_size, HEAD).astype(jnp.float32)
        new_keys = projected[:, heads_total:heads_total + kv_width].reshape(SEQS, KVH, HEAD).astype(jnp.float32)
        new_values = projected[:, heads_total + kv_width:].reshape(SEQS, KVH, HEAD).astype(jnp.float32)
        picked = pick_blocks(memory[layer_index], selected)
        cache_keys = picked[:, :, :, 0].reshape(SEQS, KVH, SEL * BLOCK, HEAD).astype(jnp.float32)
        cache_values = picked[:, :, :, 1].reshape(SEQS, KVH, SEL * BLOCK, HEAD).astype(jnp.float32)
        scores = jnp.einsum('bgrd,bgnd->bgrn', queries, cache_keys, precision=lax.Precision.HIGHEST) * score_scale
        own_score = jnp.einsum('bgrd,bgd->bgr', queries, new_keys, precision=lax.Precision.HIGHEST) * score_scale
        masked = jnp.where(live_mask[:, :, None, :], scores, FLOOR)
        top_score = jnp.maximum(lax.optimization_barrier(jnp.max(masked, axis=3)), own_score)
        weights = jnp.where(live_mask[:, :, None, :], jnp.exp(masked - top_score[..., None]), 0.0)
        own_weight = jnp.exp(own_score - top_score)
        denominator = lax.optimization_barrier(jnp.sum(weights, axis=3)) + own_weight
        numerator = jnp.einsum('bgrn,bgnd->bgrd', weights, cache_values, precision=lax.Precision.HIGHEST)
        numerator = numerator + own_weight[..., None] * new_values[:, :, None, :]
        attended = (numerator / denominator[..., None]).astype(jnp.bfloat16).reshape(SEQS, heads_total)
        branch = jnp.dot(attended, out_weight[layer_index], preferred_element_type=jnp.float32)
        current = (hidden_wide + branch).astype(jnp.bfloat16)
        hidden_list.append(current)
        attention_list.append(attended)
    return (jnp.stack(hidden_list), jnp.stack(attention_list))
```

```python
import functools

import jax
import jax.numpy as jnp
from jax import lax
from jax.experimental import pallas as pl
from jax.experimental.pallas import tpu as pltpu
from jax.sharding import Mesh
from jax.sharding import PartitionSpec as P

MESH = pl.DeviceIdType.MESH
EPSILON = 1e-05
FLOOR = -1e30
RING_X = 4
PAIR_Z = 2
SEQ = ("seq_0", "seq_1")


def places(x_size):
    found = [(dx, dz) for dx in range(x_size) for dz in range(PAIR_Z)]
    hops = [min(dx, x_size - dx) + dz for dx, dz in found]
    return found, hops


def kernel(
    sizes,
    lengths,
    hidden_in,
    gain,
    selected,
    qkv_hbm,
    out_hbm,
    memory_hbm,
    hidden_out,
    attention_out,
    w_in,
    w_out,
    mem,
    live,
    hin,
    hnew,
    part,
    part_in,
    total,
    total_in,
    query,
    local,
    local_in,
    merged,
    merged_in,
    rows,
    own_rows,
    attended,
    fetch_sem,
    hop_sem,
    send,
    recv,
):
    seqs, heads_kv, group, head, block, blocks_local, x_size, z_size = sizes
    lanes = group * head
    q_width = heads_kv * lanes
    far_size = z_size // PAIR_Z
    offsets, hops = places(x_size)
    near_first = sorted(range(1, len(offsets)), key=lambda k: hops[k])
    far_first = near_first[::-1]
    ring_far = sorted(range(1, far_size), key=lambda k: -min(k, far_size - k))

    x = lax.axis_index(SEQ[0])
    z = lax.axis_index(SEQ[1])
    section = lax.axis_index("section")
    pair = lax.rem(z, PAIR_Z)
    base_z = z - pair
    shard = x * z_size + z
    scale = head ** (-0.5)

    fetch_in = pltpu.make_async_copy(qkv_hbm.at[0], w_in, fetch_sem.at[0])
    fetch_mem = pltpu.make_async_copy(memory_hbm.at[0], mem, fetch_sem.at[1])
    fetch_out = pltpu.make_async_copy(out_hbm.at[0], w_out, fetch_sem.at[2])
    fetch_in.start()
    fetch_mem.start()
    fetch_out.start()

    def in_block(k):
        dx, dz = offsets[k]
        return lax.rem(x + dx, x_size), lax.rem(pair + dz, PAIR_Z)

    def kv_of(k):
        bx, bz = in_block(k)
        return bx * PAIR_Z + bz

    def block_device(k):
        bx, bz = in_block(k)
        return {SEQ[0]: bx, SEQ[1]: base_z + bz}

    def far_device(k):
        return {SEQ[1]: lax.rem(z + k * PAIR_Z, z_size)}

    def opposite(k):
        dx, dz = offsets[k]
        return offsets.index(((x_size - dx) % x_size, dz))

    partner = {"section": 1 - section}
    barrier = pltpu.get_barrier_semaphore()
    for k in ring_far:
        pl.semaphore_signal(barrier, inc=1, device_id=far_device(k), device_id_type=MESH)
    for k in far_first:
        pl.semaphore_signal(barrier, inc=1, device_id=block_device(k), device_id_type=MESH)
    pl.semaphore_signal(barrier, inc=1, device_id=partner, device_id_type=MESH)

    tokens = blocks_local * block
    first_block = shard * blocks_local
    lane = lax.broadcasted_iota(jnp.int32, (heads_kv, tokens), 1)
    for b in range(seqs):
        chosen_ids = selected[b]
        lane_block = first_block + lane // block
        hit = jnp.zeros((heads_kv, tokens), jnp.float32)
        for s in range(selected.shape[2]):
            hit = jnp.where(chosen_ids[:, s : s + 1] == lane_block, 1.0, hit)
        hit = jnp.where(first_block * block + lane < lengths[b], hit, 0.0)
        for g in range(heads_kv):
            live[b, g] = jnp.broadcast_to(hit[g : g + 1, :], (group, tokens))

    pl.semaphore_wait(barrier, len(ring_far) + len(far_first) + 1)

    def copy_to(stage, k, slot, source, target, device):
        return pltpu.make_async_remote_copy(
            src_ref=source,
            dst_ref=target,
            send_sem=send.at[stage, k],
            recv_sem=recv.at[stage, slot],
            device_id=device,
            device_id_type=MESH,
        )

    pending = []

    def start(copy):
        copy.start()
        pending.append(copy)

    hop = pltpu.make_async_remote_copy(
        src_ref=hnew,
        dst_ref=hin,
        send_sem=hop_sem.at[0],
        recv_sem=hop_sem.at[1],
        device_id=partner,
        device_id_type=MESH,
    )

    @pl.when(section == 0)
    def _():
        hin[...] = hidden_in[...]

    fetch_in.wait()

    @pl.when(section == 1)
    def _():
        hop.wait_recv()

    wide = hin[...].astype(jnp.float32)
    normed = (wide * gain[...].astype(jnp.float32)).astype(jnp.bfloat16)
    squares = wide * wide
    for k in [*far_first, 0]:
        g = kv_of(k)
        at_q = pl.multiple_of(g * lanes, lanes)
        at_k = pl.multiple_of(q_width + g * head, head)
        at_v = pl.multiple_of(q_width + heads_kv * head + g * head, head)
        qs = jnp.dot(normed, w_in[:, pl.ds(at_q, lanes)], preferred_element_type=jnp.float32)
        ks = jnp.dot(normed, w_in[:, pl.ds(at_k, head)], preferred_element_type=jnp.float32)
        vs = jnp.dot(normed, w_in[:, pl.ds(at_v, head)], preferred_element_type=jnp.float32)
        for b in range(seqs):
            for r in range(group):
                part[k, b, r : r + 1, :] = qs[b : b + 1, r * head : (r + 1) * head]
        part[k, seqs, 0:2, :] = ks
        part[k, seqs, 2:4, :] = vs
        part[k, seqs, 4:6, :] = squares
        part[k, seqs, 6:8, :] = jnp.zeros((2, head), jnp.float32)
        if k:
            start(copy_to(0, k, k, part.at[k], part_in.at[k], block_device(k)))

    value = part[0]
    for k in near_first:
        copy_to(0, k, k, part.at[k], part_in.at[k], block_device(k)).wait_recv()
        value = value + part_in[k]
    total[...] = value
    for k in ring_far:
        start(copy_to(1, k, k, total, total_in.at[k], far_device(k)))
    for k in ring_far[::-1]:
        copy_to(1, k, k, total, total_in.at[k], far_device(k)).wait_recv()
        value = value + total_in[k]

    model_width = hin.shape[1] * x_size * z_size
    own_q, own_k, own_v = [], [], []
    for b in range(seqs):
        mean = jnp.sum(value[seqs, 4 + b : 5 + b, :], axis=1, keepdims=True) / model_width
        inverse = lax.rsqrt(mean + EPSILON)
        q = (value[b] * inverse).astype(jnp.bfloat16)
        query[0, b] = q
        own_q.append(q.astype(jnp.float32))
        own_k.append((value[seqs, b : b + 1, :] * inverse).astype(jnp.bfloat16).astype(jnp.float32))
        own_v.append(
            (value[seqs, 2 + b : 3 + b, :] * inverse).astype(jnp.bfloat16).astype(jnp.float32)
        )
    for k in far_first:
        slot = opposite(k)
        start(copy_to(2, k, slot, query.at[0], query.at[slot], block_device(k)))
    own_score = [
        jnp.sum(own_q[b] * own_k[b], axis=1, keepdims=True) * scale for b in range(seqs)
    ]

    fetch_mem.wait()
    stat_lane = lax.broadcasted_iota(jnp.int32, (group, head), 1)

    def attend(k):
        g = kv_of(k)
        peaks, sums = [], []
        for b in range(seqs):
            keys = mem[b, g, :, 0].reshape(tokens, head)
            values = mem[b, g, :, 1].reshape(tokens, head)
            mask = live[b, g] > 0.5
            score = lax.dot_general(
                query[k, b], keys, (((1,), (1,)), ((), ())), preferred_element_type=jnp.float32
            )
            score = jnp.where(mask, score * scale, FLOOR)
            peak = jnp.max(score, axis=1, keepdims=True)
            weight = jnp.where(mask, jnp.exp(score - peak), 0.0)
            high = weight.astype(jnp.bfloat16)
            low = (weight - high.astype(jnp.float32)).astype(jnp.bfloat16)
            both = jnp.concatenate([high, low], axis=0)
            mixed = jnp.dot(both, values, preferred_element_type=jnp.float32)
            local[k, b] = mixed[:group] + mixed[group:]
            peaks.append(peak)
            sums.append(jnp.sum(weight, axis=1, keepdims=True))
        stats = sums[1]
        stats = jnp.where(stat_lane < 3, sums[0], stats)
        stats = jnp.where(stat_lane < 2, peaks[1], stats)
        local[k, seqs] = jnp.where(stat_lane < 1, peaks[0], stats)

    attend(0)
    for k in near_first:
        slot = k
        copy_to(2, k, slot, query.at[0], query.at[slot], block_device(k)).wait_recv()
        attend(k)
        start(copy_to(3, k, k, local.at[k], local_in.at[k], block_device(k)))

    def combine(parts):
        top = parts[0][seqs]
        for p in parts[1:]:
            top = jnp.maximum(top, p[seqs])
        sums = jnp.zeros((group, head), jnp.float32)
        outs = [jnp.zeros((group, head), jnp.float32) for _ in range(seqs)]
        for p in parts:
            factor = jnp.where(stat_lane < 2, jnp.exp(jnp.minimum(p[seqs] - top, 0.0)), 0.0)
            wides = [
                jnp.broadcast_to(factor[:, b : b + 1], (group, head)) for b in range(seqs)
            ]
            sums = sums + p[seqs] * jnp.where(stat_lane < 3, wides[0], wides[1])
            outs = [outs[b] + p[b] * wides[b] for b in range(seqs)]
        return outs, jnp.where(stat_lane < 2, top, sums)

    for k in near_first:
        copy_to(3, k, k, local.at[k], local_in.at[k], block_device(k)).wait_recv()
    outs, stats = combine([local[0], *[local_in[k] for k in near_first]])
    for b in range(seqs):
        merged[b] = outs[b]
    merged[seqs] = stats
    for k in ring_far:
        start(copy_to(4, k, k, merged, merged_in.at[k], far_device(k)))
    for k in ring_far[::-1]:
        copy_to(4, k, k, merged, merged_in.at[k], far_device(k)).wait_recv()
    outs, stats = combine([merged[...], *[merged_in[k] for k in ring_far]])
    for b in range(seqs):
        peak, summed = stats[:, b : b + 1], stats[:, 2 + b : 3 + b]
        top = jnp.maximum(peak, own_score[b])
        old, own = jnp.exp(peak - top), jnp.exp(own_score[b] - top)
        result = (outs[b] * old + own * own_v[b]) / (summed * old + own)
        for r in range(group):
            rows[b : b + 1, r * head : (r + 1) * head] = result[r : r + 1, :]
    own_g = kv_of(0)
    own_rows[...] = rows[...].astype(jnp.bfloat16)
    for k in far_first:
        slot = opposite(k)
        start(copy_to(5, k, slot, own_rows, attended.at[slot], block_device(k)))

    fetch_out.wait()
    branch = jnp.dot(
        own_rows[...],
        w_out[pl.ds(pl.multiple_of(own_g * lanes, lanes), lanes), :],
        preferred_element_type=jnp.float32,
    )
    attention_out[0, :, pl.ds(pl.multiple_of(own_g * lanes, lanes), lanes)] = own_rows[...]
    for k in near_first:
        copy_to(5, k, k, own_rows, attended.at[k], block_device(k)).wait_recv()
        at = pl.multiple_of(kv_of(k) * lanes, lanes)
        piece = attended[k]
        branch = branch + jnp.dot(
            piece, w_out[pl.ds(at, lanes), :], preferred_element_type=jnp.float32
        )
        attention_out[0, :, pl.ds(at, lanes)] = piece
    new = (wide + branch).astype(jnp.bfloat16)
    hidden_out[0] = new

    @pl.when(section == 0)
    def _():
        hnew[...] = new
        hop.start()
        hop.wait_send()

    for copy in pending:
        copy.wait_send()


def body(hidden_in, norm_gain, qkv_weight, out_weight, memory, lengths, selected):
    seqs, width = hidden_in.shape
    _, _, heads_kv, blocks_local, _, block, head = memory.shape
    heads_total = out_weight.shape[1]
    group = heads_total // (heads_kv * head)
    x_size, z_size = lax.axis_size(SEQ[0]), lax.axis_size(SEQ[1])
    sizes = (seqs, heads_kv, group, head, block, blocks_local, x_size, z_size)
    members = x_size * PAIR_Z
    far = z_size // PAIR_Z
    tile = (seqs + 1, group, head)
    f32, bf16 = jnp.float32, jnp.bfloat16
    vmem = pl.BlockSpec(memory_space=pltpu.VMEM)
    hbm = pl.BlockSpec(memory_space=pl.ANY)
    slots = max(members, far)
    return pl.pallas_call(
        functools.partial(kernel, sizes),
        out_shape=(
            jax.ShapeDtypeStruct((1, seqs, width), bf16),
            jax.ShapeDtypeStruct((1, seqs, heads_total), bf16),
        ),
        in_specs=[pl.BlockSpec(memory_space=pltpu.SMEM), vmem, vmem, vmem, hbm, hbm, hbm],
        out_specs=(vmem, vmem),
        scratch_shapes=[
            pltpu.VMEM(qkv_weight.shape[1:], bf16),
            pltpu.VMEM(out_weight.shape[1:], bf16),
            pltpu.VMEM(memory.shape[1:], bf16),
            pltpu.VMEM((seqs, heads_kv, group, blocks_local * block), f32),
            pltpu.VMEM((seqs, width), bf16),
            pltpu.VMEM((seqs, width), bf16),
            pltpu.VMEM((members, *tile), f32),
            pltpu.VMEM((members, *tile), f32),
            pltpu.VMEM(tile, f32),
            pltpu.VMEM((far, *tile), f32),
            pltpu.VMEM((members, seqs, group, head), bf16),
            pltpu.VMEM((members, *tile), f32),
            pltpu.VMEM((members, *tile), f32),
            pltpu.VMEM(tile, f32),
            pltpu.VMEM((far, *tile), f32),
            pltpu.VMEM((seqs, group * head), f32),
            pltpu.VMEM((seqs, group * head), bf16),
            pltpu.VMEM((members, seqs, group * head), bf16),
            pltpu.SemaphoreType.DMA((3,)),
            pltpu.SemaphoreType.DMA((2,)),
            pltpu.SemaphoreType.DMA((6, slots)),
            pltpu.SemaphoreType.DMA((6, slots)),
        ],
        compiler_params=pltpu.CompilerParams(collective_id=0, has_side_effects=True),
        name="decode",
    )(lengths, hidden_in, norm_gain, selected, qkv_weight, out_weight, memory)


def solution(mesh):
    z_size = mesh.shape["seq"] // RING_X
    finer = Mesh(
        mesh.devices.reshape(mesh.shape["groups"], RING_X, z_size, mesh.shape["section"]),
        ("groups", *SEQ, "section"),
    )
    in_specs = (
        P("groups", SEQ),
        P("section", SEQ),
        P("section", SEQ, None),
        P("section", None, SEQ),
        P("section", "groups", None, SEQ, None, None, None),
        P("groups"),
        P("groups", None, None),
    )
    out_specs = (P("section", "groups", SEQ), P("section", "groups", None))
    return jax.shard_map(body, mesh=finer, in_specs=in_specs, out_specs=out_specs, check_vma=False)
```

```python
import functools

import jax
import jax.numpy as jnp
from jax import lax
from jax.experimental import pallas as pl
from jax.experimental.pallas import tpu as pltpu
from jax.sharding import Mesh
from jax.sharding import PartitionSpec as P

MESH = pl.DeviceIdType.MESH
EPSILON = 1e-05
FLOOR = -1e30
RING_X = 4
PAIR_Z = 2
SEQ = ("seq_0", "seq_1")
F32, BF16 = jnp.float32, jnp.bfloat16


def kernel(
    sizes,
    lengths_hbm,
    hidden_hbm,
    gain_hbm,
    selected_hbm,
    qkv_hbm,
    out_hbm,
    memory_hbm,
    result,
    lengths,
    selected,
    gain,
    hin,
    w_in,
    w_out,
    w_out_near,
    mem,
    mem_near,
    live,
    part,
    part_in,
    total,
    total_in,
    query,
    local,
    local_in,
    merged,
    merged_in,
    rows,
    own_rows,
    attended,
    done,
    done_in,
    fetch_sem,
    cast_sem,
    send,
    recv,
):
    seqs, heads_kv, group, head, block, blocks_local, x_size, z_size = sizes
    lanes = group * head
    q_width = heads_kv * lanes
    kv_width = heads_kv * head
    tokens = blocks_local * block
    far_size = z_size // PAIR_Z
    offsets = [(dx, dz) for dx in range(x_size) for dz in range(PAIR_Z)]
    hops = [min(dx, x_size - dx) + dz for dx, dz in offsets]
    near_first = sorted(range(1, len(offsets)), key=lambda k: hops[k])
    far_first = near_first[::-1]
    ring_far = sorted(range(1, far_size), key=lambda k: -min(k, far_size - k))

    x = lax.axis_index(SEQ[0])
    z = lax.axis_index(SEQ[1])
    section = lax.axis_index("section")
    pair = lax.rem(z, PAIR_Z)
    base_z = z - pair
    first_block = (x * z_size + z) * blocks_local
    scale = head ** (-0.5)
    model_width = hin.shape[2] * x_size * z_size

    def in_block(k):
        dx, dz = offsets[k]
        return lax.rem(x + dx, x_size), lax.rem(pair + dz, PAIR_Z)

    def kv_of(k):
        bx, bz = in_block(k)
        return bx * PAIR_Z + bz

    def block_device(k, core):
        bx, bz = in_block(k)
        return {SEQ[0]: bx, SEQ[1]: base_z + bz, "section": core}

    def far_device(k):
        return {SEQ[1]: lax.rem(z + k * PAIR_Z, z_size)}

    def opposite(k):
        dx, dz = offsets[k]
        return offsets.index(((x_size - dx) % x_size, dz))

    barrier = pltpu.get_barrier_semaphore()

    def greet(device):
        pl.semaphore_signal(barrier, inc=1, device_id=device, device_id_type=MESH)

    def copy_to(stage, k, slot, source, target, device):
        return pltpu.make_async_remote_copy(
            src_ref=source,
            dst_ref=target,
            send_sem=send.at[stage, k],
            recv_sem=recv.at[stage, slot],
            device_id=device,
            device_id_type=MESH,
        )

    def cast(number, source, target, core):
        return pltpu.make_async_remote_copy(
            src_ref=source,
            dst_ref=target,
            send_sem=cast_sem.at[0, number],
            recv_sem=cast_sem.at[1, number],
            device_id={"section": core},
            device_id_type=MESH,
        )

    cast_hidden = cast(0, hidden_hbm, hin.at[1], 1)
    cast_mem = cast(1, memory_hbm.at[0], mem_near, 1)
    cast_out = cast(2, out_hbm.at[0], w_out_near, 1)
    cast_done = cast(3, done, done_in, 0)

    fetch_gain = pltpu.make_async_copy(gain_hbm, gain, fetch_sem.at[0])
    fetch_hidden = pltpu.make_async_copy(hidden_hbm, hin.at[0], fetch_sem.at[1])
    fetch_kv = pltpu.make_async_copy(
        qkv_hbm.at[0, :, pl.ds(q_width, 2 * kv_width)],
        w_in.at[:, pl.ds(q_width, 2 * kv_width)],
        fetch_sem.at[2],
    )

    def q_columns(k):
        return pl.ds(pl.multiple_of(kv_of(k) * lanes, lanes), lanes)

    def fetch_q(k):
        return pltpu.make_async_copy(
            qkv_hbm.at[0, :, q_columns(k)], w_in.at[:, q_columns(k)], fetch_sem.at[8 + k]
        )

    fetch_selected = pltpu.make_async_copy(selected_hbm, selected, fetch_sem.at[3])
    fetch_lengths = pltpu.make_async_copy(lengths_hbm, lengths, fetch_sem.at[4])
    fetch_mem = pltpu.make_async_copy(memory_hbm.at[0], mem, fetch_sem.at[5])
    fetch_out = pltpu.make_async_copy(out_hbm.at[0], w_out, fetch_sem.at[6])

    @pl.when(section == 0)
    def _():
        greet({"section": 1})

    @pl.when(section == 1)
    def _():
        for k in [*far_first, 0]:
            greet(block_device(k, 0))
        for k in ring_far:
            greet(far_device(k))
        for k in far_first:
            greet(block_device(k, 1))

    fetch_gain.start()

    @pl.when(section == 0)
    def _():
        fetch_hidden.start()

    fetch_kv.start()
    for k in [*far_first, 0]:
        fetch_q(k).start()

    def project(wide, ready, send_one):
        normed = (wide * gain[...].astype(F32)).astype(BF16)
        squares = wide * wide
        for k in [*far_first, 0]:
            g = kv_of(k)
            at_k = pl.multiple_of(q_width + g * head, head)
            at_v = pl.multiple_of(q_width + kv_width + g * head, head)
            ready(k)
            qs = jnp.dot(normed, w_in[:, q_columns(k)], preferred_element_type=F32)
            ks = jnp.dot(normed, w_in[:, pl.ds(at_k, head)], preferred_element_type=F32)
            vs = jnp.dot(normed, w_in[:, pl.ds(at_v, head)], preferred_element_type=F32)
            for b in range(seqs):
                for r in range(group):
                    part[k, b, r : r + 1, :] = qs[b : b + 1, r * head : (r + 1) * head]
            part[k, seqs, 0:2, :] = ks
            part[k, seqs, 2:4, :] = vs
            part[k, seqs, 4:6, :] = squares
            part[k, seqs, 6:8, :] = jnp.zeros((2, head), F32)
            send_one(k)

    @pl.when(section == 0)
    def _():
        fetch_gain.wait()
        fetch_hidden.wait()
        fetch_kv.wait()
        sent = []

        def send_one(k):
            if not sent:
                pl.semaphore_wait(barrier, len(offsets))
            copy = copy_to(0, k, k, part.at[k], part_in.at[0, k], block_device(k, 1))
            copy.start()
            sent.append(copy)

        project(hin[0].astype(F32), lambda k: fetch_q(k).wait(), send_one)
        cast_hidden.start()
        cast_mem.start()
        cast_out.start()
        for copy in [*sent, cast_hidden, cast_mem, cast_out]:
            copy.wait_send()
        cast_done.wait_recv()
        result[0] = done_in[...]

    @pl.when(section == 1)
    def _():
        fetch_selected.start()
        fetch_lengths.start()
        fetch_mem.start()
        fetch_out.start()

        fetch_selected.wait()
        fetch_lengths.wait()
        lane = lax.broadcasted_iota(jnp.int32, (heads_kv, tokens), 1)
        for b in range(seqs):
            chosen_ids = selected[b]
            lane_block = first_block + lane // block
            hit = jnp.zeros((heads_kv, tokens), F32)
            for s in range(selected.shape[2]):
                hit = jnp.where(chosen_ids[:, s : s + 1] == lane_block, 1.0, hit)
            hit = jnp.where(first_block * block + lane < lengths[b], hit, 0.0)
            for g in range(heads_kv):
                live[b, g] = jnp.broadcast_to(hit[g : g + 1, :], (group, tokens))
        stat_lane = lax.broadcasted_iota(jnp.int32, (group, head), 1)
        pending = []

        def start(copy):
            copy.start()
            pending.append(copy)

        def attend(layer, k, memory):
            g = kv_of(k)
            peaks, sums = [], []
            for b in range(seqs):
                keys = memory[b, g, :, 0].reshape(tokens, head)
                values = memory[b, g, :, 1].reshape(tokens, head)
                mask = live[b, g] > 0.5
                score = lax.dot_general(
                    query[layer, k, b], keys, (((1,), (1,)), ((), ())), preferred_element_type=F32
                )
                score = jnp.where(mask, score * scale, FLOOR)
                peak = jnp.max(score, axis=1, keepdims=True)
                weight = jnp.where(mask, jnp.exp(score - peak), 0.0)
                high = weight.astype(BF16)
                low = (weight - high.astype(F32)).astype(BF16)
                both = jnp.concatenate([high, low], axis=0)
                mixed = jnp.dot(both, values, preferred_element_type=F32)
                local[layer, k, b] = mixed[:group] + mixed[group:]
                peaks.append(peak)
                sums.append(jnp.sum(weight, axis=1, keepdims=True))
            stats = sums[1]
            stats = jnp.where(stat_lane < 3, sums[0], stats)
            stats = jnp.where(stat_lane < 2, peaks[1], stats)
            local[layer, k, seqs] = jnp.where(stat_lane < 1, peaks[0], stats)

        def combine(parts):
            top = parts[0][seqs]
            for p in parts[1:]:
                top = jnp.maximum(top, p[seqs])
            sums = jnp.zeros((group, head), F32)
            outs = [jnp.zeros((group, head), F32) for _ in range(seqs)]
            for p in parts:
                factor = jnp.where(stat_lane < 2, jnp.exp(jnp.minimum(p[seqs] - top, 0.0)), 0.0)
                wides = [
                    jnp.broadcast_to(factor[:, b : b + 1], (group, head)) for b in range(seqs)
                ]
                sums = sums + p[seqs] * jnp.where(stat_lane < 3, wides[0], wides[1])
                outs = [outs[b] + p[b] * wides[b] for b in range(seqs)]
            return outs, jnp.where(stat_lane < 2, top, sums)

        def after_projection(layer, value, wide_of, memory, memory_ready, weights, weights_ready):
            stage = 6 * layer
            total[layer] = value
            if layer == 0:
                pl.semaphore_wait(barrier, len(ring_far) + len(far_first) + 1)

            def far_copy(n, k, source, target):
                return copy_to(stage + n, k, k, source, target, far_device(k))

            def block_copy(n, k, slot, source, target):
                return copy_to(stage + n, k, slot, source, target, block_device(k, 1))

            for k in ring_far:
                start(far_copy(1, k, total.at[layer], total_in.at[layer, k]))
            for k in ring_far[::-1]:
                far_copy(1, k, total.at[layer], total_in.at[layer, k]).wait_recv()
                value = value + total_in[layer, k]

            own_q, own_k, own_v = [], [], []
            for b in range(seqs):
                mean = jnp.sum(value[seqs, 4 + b : 5 + b, :], axis=1, keepdims=True) / model_width
                inverse = lax.rsqrt(mean + EPSILON)
                q = (value[b] * inverse).astype(BF16)
                query[layer, 0, b] = q
                own_q.append(q.astype(F32))
                own_k.append((value[seqs, b : b + 1, :] * inverse).astype(BF16).astype(F32))
                own_v.append((value[seqs, 2 + b : 3 + b, :] * inverse).astype(BF16).astype(F32))
            for k in far_first:
                slot = opposite(k)
                start(block_copy(2, k, slot, query.at[layer, 0], query.at[layer, slot]))
            own_score = [
                jnp.sum(own_q[b] * own_k[b], axis=1, keepdims=True) * scale for b in range(seqs)
            ]

            memory_ready()
            attend(layer, 0, memory)
            for k in near_first:
                block_copy(2, k, k, query.at[layer, 0], query.at[layer, k]).wait_recv()
                attend(layer, k, memory)
                start(block_copy(3, k, k, local.at[layer, k], local_in.at[layer, k]))
            for k in near_first:
                block_copy(3, k, k, local.at[layer, k], local_in.at[layer, k]).wait_recv()
            outs, stats = combine([local[layer, 0], *[local_in[layer, k] for k in near_first]])
            for b in range(seqs):
                merged[layer, b] = outs[b]
            merged[layer, seqs] = stats
            for k in ring_far:
                start(far_copy(4, k, merged.at[layer], merged_in.at[layer, k]))
            for k in ring_far[::-1]:
                far_copy(4, k, merged.at[layer], merged_in.at[layer, k]).wait_recv()
            outs, stats = combine([merged[layer], *[merged_in[layer, k] for k in ring_far]])
            for b in range(seqs):
                peak, summed = stats[:, b : b + 1], stats[:, 2 + b : 3 + b]
                top = jnp.maximum(peak, own_score[b])
                old, own = jnp.exp(peak - top), jnp.exp(own_score[b] - top)
                shared = (outs[b] * old + own * own_v[b]) / (summed * old + own)
                for r in range(group):
                    rows[b : b + 1, r * head : (r + 1) * head] = shared[r : r + 1, :]
            own_rows[layer] = rows[...].astype(BF16)
            for k in far_first:
                slot = opposite(k)
                start(block_copy(5, k, slot, own_rows.at[layer], attended.at[layer, slot]))

            weights_ready()
            branch = jnp.zeros((seqs, done.shape[1] - q_width), F32)
            for k in [0, *near_first]:
                if k:
                    block_copy(5, k, k, own_rows.at[layer], attended.at[layer, k]).wait_recv()
                piece = attended[layer, k] if k else own_rows[layer]
                branch = branch + jnp.dot(
                    piece, weights[q_columns(k), :], preferred_element_type=F32
                )
                if layer == 0:
                    done[:, q_columns(k)] = piece
                else:
                    result[0, :, q_columns(k)] = piece
            return (wide_of() + branch).astype(BF16)

        value = None
        for k in [0, *near_first]:
            copy_to(0, k, k, part.at[k], part_in.at[0, k], block_device(k, 1)).wait_recv()
            value = part_in[0, k] if value is None else value + part_in[0, k]

        def first_hidden():
            cast_hidden.wait_recv()
            return hin[1].astype(F32)

        new = after_projection(
            0, value, first_hidden, mem_near, cast_mem.wait_recv, w_out_near, cast_out.wait_recv
        )
        done[:, q_width:] = new
        fetch_gain.wait()
        fetch_kv.wait()
        for k in [*far_first, 0]:
            fetch_q(k).wait()
        wide = new.astype(F32)

        def send_one(k):
            if k:
                start(copy_to(6, k, k, part.at[k], part_in.at[1, k], block_device(k, 1)))

        project(wide, lambda k: None, send_one)
        start(cast_done)
        value = part[0]
        for k in near_first:
            copy_to(6, k, k, part.at[k], part_in.at[1, k], block_device(k, 1)).wait_recv()
            value = value + part_in[1, k]
        new = after_projection(1, value, lambda: wide, mem, fetch_mem.wait, w_out, fetch_out.wait)
        result[0, :, q_width:] = new
        for copy in pending:
            copy.wait_send()


def body(hidden_in, norm_gain, qkv_weight, out_weight, memory, lengths, selected):
    seqs, width = hidden_in.shape
    _, _, heads_kv, blocks_local, _, block, head = memory.shape
    heads_total = out_weight.shape[1]
    group = heads_total // (heads_kv * head)
    x_size, z_size = lax.axis_size(SEQ[0]), lax.axis_size(SEQ[1])
    sizes = (seqs, heads_kv, group, head, block, blocks_local, x_size, z_size)
    members = x_size * PAIR_Z
    far = z_size // PAIR_Z
    tile = (seqs + 1, group, head)
    hbm = pl.BlockSpec(memory_space=pl.ANY)
    slots = max(members, far)
    result = pl.pallas_call(
        functools.partial(kernel, sizes),
        out_shape=jax.ShapeDtypeStruct((1, seqs, heads_total + width), BF16),
        in_specs=[hbm] * 7,
        out_specs=pl.BlockSpec(memory_space=pltpu.VMEM),
        scratch_shapes=[
            pltpu.SMEM(lengths.shape, jnp.int32),
            pltpu.VMEM(selected.shape, jnp.int32),
            pltpu.VMEM((1, width), BF16),
            pltpu.VMEM((2, seqs, width), BF16),
            pltpu.VMEM(qkv_weight.shape[1:], BF16),
            pltpu.VMEM(out_weight.shape[1:], BF16),
            pltpu.VMEM(out_weight.shape[1:], BF16),
            pltpu.VMEM(memory.shape[1:], BF16),
            pltpu.VMEM(memory.shape[1:], BF16),
            pltpu.VMEM((seqs, heads_kv, group, blocks_local * block), F32),
            pltpu.VMEM((members, *tile), F32),
            pltpu.VMEM((2, members, *tile), F32),
            pltpu.VMEM((2, *tile), F32),
            pltpu.VMEM((2, far, *tile), F32),
            pltpu.VMEM((2, members, seqs, group, head), BF16),
            pltpu.VMEM((2, members, *tile), F32),
            pltpu.VMEM((2, members, *tile), F32),
            pltpu.VMEM((2, *tile), F32),
            pltpu.VMEM((2, far, *tile), F32),
            pltpu.VMEM((seqs, group * head), F32),
            pltpu.VMEM((2, seqs, group * head), BF16),
            pltpu.VMEM((2, members, seqs, group * head), BF16),
            pltpu.VMEM((seqs, heads_total + width), BF16),
            pltpu.VMEM((seqs, heads_total + width), BF16),
            pltpu.SemaphoreType.DMA((8 + members,)),
            pltpu.SemaphoreType.DMA((2, 4)),
            pltpu.SemaphoreType.DMA((12, slots)),
            pltpu.SemaphoreType.DMA((12, slots)),
        ],
        compiler_params=pltpu.CompilerParams(collective_id=0, has_side_effects=True),
        name="decode",
    )(lengths, hidden_in, norm_gain, selected, qkv_weight, out_weight, memory)
    return result[:, :, heads_total:], result[:, :, :heads_total]


def solution(mesh):
    z_size = mesh.shape["seq"] // RING_X
    finer = Mesh(
        mesh.devices.reshape(mesh.shape["groups"], RING_X, z_size, mesh.shape["section"]),
        ("groups", *SEQ, "section"),
    )
    in_specs = (
        P("groups", SEQ),
        P("section", SEQ),
        P("section", SEQ, None),
        P("section", None, SEQ),
        P("section", "groups", None, SEQ, None, None, None),
        P("groups"),
        P("groups", None, None),
    )
    out_specs = (P("section", "groups", SEQ), P("section", "groups", None))
    return jax.shard_map(body, mesh=finer, in_specs=in_specs, out_specs=out_specs, check_vma=False)
```

```python
import functools

import jax
import jax.numpy as jnp
from jax import lax
from jax.experimental import pallas as pl
from jax.experimental.pallas import tpu as pltpu
from jax.sharding import Mesh
from jax.sharding import PartitionSpec as P

MESH = pl.DeviceIdType.MESH
EPSILON = 1e-05
FLOOR = -1e30
RING_X = 4
PAIR_Z = 2
SEQ = ("seq_0", "seq_1")
F32, BF16 = jnp.float32, jnp.bfloat16
VMEM_BYTES = 64000000


def kernel(
    sizes,
    lengths_hbm,
    hidden_hbm,
    gain_hbm,
    selected_hbm,
    qkv_hbm,
    out_hbm,
    memory_hbm,
    result,
    lengths,
    selected,
    gain,
    hin,
    w_in,
    w_out,
    w_out_near,
    mem_stage,
    mem_block,
    mem_near,
    live,
    live_block,
    part,
    part_in,
    total,
    total_in,
    query,
    local,
    local_in,
    merged,
    merged_in,
    rows,
    own_rows,
    attended,
    done,
    done_in,
    fetch_sem,
    cast_sem,
    ready_sem,
    group_sem,
    send,
    recv,
):
    seqs, heads_kv, group, head, block, blocks_local, x_size, z_size = sizes
    lanes = group * head
    q_width = heads_kv * lanes
    kv_width = heads_kv * head
    tokens = blocks_local * block
    far_size = z_size // PAIR_Z
    offsets = [(dx, dz) for dx in range(x_size) for dz in range(PAIR_Z)]
    hops = [min(dx, x_size - dx) + dz for dx, dz in offsets]
    near_first = sorted(range(1, len(offsets)), key=lambda k: hops[k])
    far_first = near_first[::-1]
    ring_far = sorted(range(1, far_size), key=lambda k: -min(k, far_size - k))

    x = lax.axis_index(SEQ[0])
    z = lax.axis_index(SEQ[1])
    section = lax.axis_index("section")
    pair = lax.rem(z, PAIR_Z)
    base_z = z - pair
    first_block = (x * z_size + z) * blocks_local
    scale = head ** (-0.5)
    model_width = hin.shape[2] * x_size * z_size

    def in_block(k):
        dx, dz = offsets[k]
        return lax.rem(x + dx, x_size), lax.rem(pair + dz, PAIR_Z)

    def kv_of(k):
        bx, bz = in_block(k)
        return bx * PAIR_Z + bz

    def block_device(k, core):
        bx, bz = in_block(k)
        return {SEQ[0]: bx, SEQ[1]: base_z + bz, "section": core}

    def far_device(k):
        return {SEQ[1]: lax.rem(z + k * PAIR_Z, z_size)}

    def opposite(k):
        dx, dz = offsets[k]
        return offsets.index(((x_size - dx) % x_size, dz))

    barrier = pltpu.get_barrier_semaphore()

    def greet(device):
        pl.semaphore_signal(barrier, inc=1, device_id=device, device_id_type=MESH)

    def copy_to(stage, k, slot, source, target, device):
        return pltpu.make_async_remote_copy(
            src_ref=source,
            dst_ref=target,
            send_sem=send.at[stage, k],
            recv_sem=recv.at[stage, slot],
            device_id=device,
            device_id_type=MESH,
        )

    def cast(number, source, target, core):
        return pltpu.make_async_remote_copy(
            src_ref=source,
            dst_ref=target,
            send_sem=cast_sem.at[0, number],
            recv_sem=cast_sem.at[1, number],
            device_id={"section": core},
            device_id_type=MESH,
        )

    def stage_memory(k):
        return pltpu.make_async_remote_copy(
            src_ref=memory_hbm.at[0, :, kv_of(k)],
            dst_ref=mem_stage.at[k],
            send_sem=group_sem.at[0, k],
            recv_sem=group_sem.at[1, k],
            device_id={"section": 0},
            device_id_type=MESH,
        )

    def regroup(k, slot):
        return pltpu.make_async_remote_copy(
            src_ref=mem_stage.at[k],
            dst_ref=mem_block.at[slot],
            send_sem=group_sem.at[2, k],
            recv_sem=group_sem.at[3, slot],
            device_id=block_device(k, 1),
            device_id_type=MESH,
        )

    cast_hidden = cast(0, hidden_hbm, hin.at[1], 1)
    cast_mem = cast(1, memory_hbm.at[0], mem_near, 1)
    cast_out = cast(2, out_hbm.at[0], w_out_near, 1)
    cast_done = cast(3, done, done_in, 0)

    fetch_gain = pltpu.make_async_copy(gain_hbm, gain, fetch_sem.at[0])
    fetch_hidden = pltpu.make_async_copy(hidden_hbm, hin.at[0], fetch_sem.at[1])
    fetch_kv = pltpu.make_async_copy(
        qkv_hbm.at[0, :, pl.ds(q_width, 2 * kv_width)],
        w_in.at[:, pl.ds(q_width, 2 * kv_width)],
        fetch_sem.at[2],
    )

    def q_columns(k):
        return pl.ds(pl.multiple_of(kv_of(k) * lanes, lanes), lanes)

    def fetch_q(k):
        return pltpu.make_async_copy(
            qkv_hbm.at[0, :, q_columns(k)], w_in.at[:, q_columns(k)], fetch_sem.at[8 + k]
        )

    fetch_selected = pltpu.make_async_copy(selected_hbm, selected, fetch_sem.at[3])
    fetch_lengths = pltpu.make_async_copy(lengths_hbm, lengths, fetch_sem.at[4])
    fetch_mem = pltpu.make_async_copy(
        memory_hbm.at[0, :, kv_of(0)], mem_block.at[0], fetch_sem.at[5]
    )
    fetch_out = pltpu.make_async_copy(out_hbm.at[0], w_out, fetch_sem.at[6])

    @pl.when(section == 0)
    def _():
        greet({"section": 1})

    @pl.when(section == 1)
    def _():
        for k in [*far_first, 0]:
            greet(block_device(k, 0))
        for k in ring_far:
            greet(far_device(k))
        for k in far_first:
            greet(block_device(k, 1))

    fetch_gain.start()

    @pl.when(section == 0)
    def _():
        fetch_hidden.start()

    fetch_kv.start()
    for k in [*far_first, 0]:
        fetch_q(k).start()

    def project(wide, ready, send_one):
        normed = (wide * gain[...].astype(F32)).astype(BF16)
        squares = wide * wide
        for k in [*far_first, 0]:
            g = kv_of(k)
            at_k = pl.multiple_of(q_width + g * head, head)
            at_v = pl.multiple_of(q_width + kv_width + g * head, head)
            ready(k)
            qs = jnp.dot(normed, w_in[:, q_columns(k)], preferred_element_type=F32)
            ks = jnp.dot(normed, w_in[:, pl.ds(at_k, head)], preferred_element_type=F32)
            vs = jnp.dot(normed, w_in[:, pl.ds(at_v, head)], preferred_element_type=F32)
            for b in range(seqs):
                for r in range(group):
                    part[k, b, r : r + 1, :] = qs[b : b + 1, r * head : (r + 1) * head]
            part[k, seqs, 0:2, :] = ks
            part[k, seqs, 2:4, :] = vs
            part[k, seqs, 4:6, :] = squares
            part[k, seqs, 6:8, :] = jnp.zeros((2, head), F32)
            send_one(k)

    @pl.when(section == 0)
    def _():
        fetch_gain.wait()
        fetch_hidden.wait()
        fetch_kv.wait()
        sent = []

        def send_one(k):
            if not sent:
                pl.semaphore_wait(barrier, len(offsets))
                pl.semaphore_signal(
                    ready_sem, inc=1, device_id={"section": 1}, device_id_type=MESH
                )
            copy = copy_to(0, k, k, part.at[k], part_in.at[0, k], block_device(k, 1))
            copy.start()
            sent.append(copy)

        project(hin[0].astype(F32), lambda k: fetch_q(k).wait(), send_one)
        cast_hidden.start()
        cast_mem.start()
        cast_out.start()
        for k in far_first:
            stage_memory(k).wait_recv()
            copy = regroup(k, opposite(k))
            copy.start()
            sent.append(copy)
        for copy in [*sent, cast_hidden, cast_mem, cast_out]:
            copy.wait_send()
        cast_done.wait_recv()
        result[0] = done_in[...]

    @pl.when(section == 1)
    def _():
        pending = []

        def start(copy):
            copy.start()
            pending.append(copy)

        fetch_selected.start()
        fetch_lengths.start()
        fetch_mem.start()
        fetch_out.start()

        fetch_selected.wait()
        fetch_lengths.wait()
        lane = lax.broadcasted_iota(jnp.int32, (heads_kv, tokens), 1)
        for b in range(seqs):
            chosen_ids = selected[b]
            lane_block = first_block + lane // block
            hit = jnp.zeros((heads_kv, tokens), F32)
            for s in range(selected.shape[2]):
                hit = jnp.where(chosen_ids[:, s : s + 1] == lane_block, 1.0, hit)
            hit = jnp.where(first_block * block + lane < lengths[b], hit, 0.0)
            for g in range(heads_kv):
                live[b, g] = jnp.broadcast_to(hit[g : g + 1, :], (group, tokens))

        pl.semaphore_wait(ready_sem, 1)
        for k in far_first:
            start(stage_memory(k))

        row = lax.broadcasted_iota(jnp.int32, (len(offsets), tokens), 0)
        row_lane = lax.broadcasted_iota(jnp.int32, (len(offsets), tokens), 1)
        row_first = jnp.zeros((len(offsets), tokens), jnp.int32)
        for k in range(len(offsets)):
            bx, bz = in_block(k)
            row_first = jnp.where(
                row == k, (bx * z_size + base_z + bz) * blocks_local, row_first
            )
        for b in range(seqs):
            chosen_ids = selected[b, pl.ds(kv_of(0), 1), :]
            hit = jnp.zeros((len(offsets), tokens), F32)
            for s in range(selected.shape[2]):
                hit = jnp.where(
                    chosen_ids[:, s : s + 1] == row_first + row_lane // block, 1.0, hit
                )
            hit = jnp.where(row_first * block + row_lane < lengths[b], hit, 0.0)
            for k in range(len(offsets)):
                live_block[b, k] = jnp.broadcast_to(hit[k : k + 1, :], (group, tokens))
        stat_lane = lax.broadcasted_iota(jnp.int32, (group, head), 1)
        def score_of(q, keys, mask):
            score = lax.dot_general(
                q, keys, (((1,), (1,)), ((), ())), preferred_element_type=F32
            )
            return jnp.where(mask, score * scale, FLOOR)

        def mix(weight, values):
            high = weight.astype(BF16)
            low = (weight - high.astype(F32)).astype(BF16)
            mixed = jnp.dot(
                jnp.concatenate([high, low], axis=0), values, preferred_element_type=F32
            )
            return mixed[:group] + mixed[group:]

        def stats_of(peaks, sums):
            stats = jnp.where(stat_lane < 3, sums[0], sums[1])
            stats = jnp.where(stat_lane < 2, peaks[1], stats)
            return jnp.where(stat_lane < 1, peaks[0], stats)

        def attend(layer, ks, memory):
            pairs = [(k, b) for k in ks for b in range(seqs)]
            heads = [kv_of(k) for k, b in pairs]
            masks = [live[b, g] > 0.5 for (k, b), g in zip(pairs, heads)]
            scores = [
                score_of(query[layer, k, b], memory[b, g, :, 0].reshape(tokens, head), mask)
                for (k, b), g, mask in zip(pairs, heads, masks)
            ]
            peaks = [jnp.max(score, axis=1, keepdims=True) for score in scores]
            weights = [
                jnp.where(mask, jnp.exp(score - peak), 0.0)
                for score, peak, mask in zip(scores, peaks, masks)
            ]
            sums = [jnp.sum(weight, axis=1, keepdims=True) for weight in weights]
            for (k, b), g, weight in zip(pairs, heads, weights):
                local[layer, k, b] = mix(weight, memory[b, g, :, 1].reshape(tokens, head))
            for n, k in enumerate(ks):
                at = slice(n * seqs, (n + 1) * seqs)
                local[layer, k, seqs] = stats_of(peaks[at], sums[at])

        def attend_block(layer):
            members = range(len(offsets))
            outs, peaks, sums = [], [], []
            for b in range(seqs):
                masks = [live_block[b, k] > 0.5 for k in members]
                scores = [
                    score_of(
                        query[layer, 0, b], mem_block[k, b, :, 0].reshape(tokens, head), masks[k]
                    )
                    for k in members
                ]
                highest = scores[0]
                for score in scores[1:]:
                    highest = jnp.maximum(highest, score)
                peak = jnp.max(highest, axis=1, keepdims=True)
                out = jnp.zeros((group, head), F32)
                total_weight = jnp.zeros((group, tokens), F32)
                for k in members:
                    weight = jnp.where(masks[k], jnp.exp(scores[k] - peak), 0.0)
                    total_weight = total_weight + weight
                    out = out + mix(weight, mem_block[k, b, :, 1].reshape(tokens, head))
                outs.append(out)
                peaks.append(peak)
                sums.append(jnp.sum(total_weight, axis=1, keepdims=True))
            return outs, stats_of(peaks, sums)

        def combine(parts):
            top = parts[0][seqs]
            for p in parts[1:]:
                top = jnp.maximum(top, p[seqs])
            sums = jnp.zeros((group, head), F32)
            outs = [jnp.zeros((group, head), F32) for _ in range(seqs)]
            for p in parts:
                factor = jnp.where(stat_lane < 2, jnp.exp(jnp.minimum(p[seqs] - top, 0.0)), 0.0)
                wides = [
                    jnp.broadcast_to(factor[:, b : b + 1], (group, head)) for b in range(seqs)
                ]
                sums = sums + p[seqs] * jnp.where(stat_lane < 3, wides[0], wides[1])
                outs = [outs[b] + p[b] * wides[b] for b in range(seqs)]
            return outs, jnp.where(stat_lane < 2, top, sums)

        def after_projection(layer, value, wide_of, memory_ready, weights, weights_ready):
            stage = 6 * layer
            total[layer] = value
            if layer == 0:
                pl.semaphore_wait(barrier, len(ring_far) + len(far_first) + 1)

            def far_copy(n, k, source, target):
                return copy_to(stage + n, k, k, source, target, far_device(k))

            def block_copy(n, k, slot, source, target):
                return copy_to(stage + n, k, slot, source, target, block_device(k, 1))

            for k in ring_far:
                start(far_copy(1, k, total.at[layer], total_in.at[layer, k]))
            for k in ring_far[::-1]:
                far_copy(1, k, total.at[layer], total_in.at[layer, k]).wait_recv()
                value = value + total_in[layer, k]

            own_q, own_k, own_v = [], [], []
            for b in range(seqs):
                mean = jnp.sum(value[seqs, 4 + b : 5 + b, :], axis=1, keepdims=True) / model_width
                inverse = lax.rsqrt(mean + EPSILON)
                q = (value[b] * inverse).astype(BF16)
                query[layer, 0, b] = q
                own_q.append(q.astype(F32))
                own_k.append((value[seqs, b : b + 1, :] * inverse).astype(BF16).astype(F32))
                own_v.append((value[seqs, 2 + b : 3 + b, :] * inverse).astype(BF16).astype(F32))
            if layer == 0:
                for k in far_first:
                    slot = opposite(k)
                    start(block_copy(2, k, slot, query.at[layer, 0], query.at[layer, slot]))
            own_score = [
                jnp.sum(own_q[b] * own_k[b], axis=1, keepdims=True) * scale for b in range(seqs)
            ]

            memory_ready()
            if layer == 0:
                attend(layer, [0], mem_near)
                for distance in sorted({hops[k] for k in near_first}):
                    batch = [k for k in near_first if hops[k] == distance]
                    for k in batch:
                        block_copy(2, k, k, query.at[layer, 0], query.at[layer, k]).wait_recv()
                    attend(layer, batch, mem_near)
                    for k in batch:
                        start(block_copy(3, k, k, local.at[layer, k], local_in.at[layer, k]))
                for k in near_first:
                    block_copy(3, k, k, local.at[layer, k], local_in.at[layer, k]).wait_recv()
                outs, stats = combine([local[layer, 0], *[local_in[layer, k] for k in near_first]])
            else:
                outs, stats = attend_block(layer)
            for b in range(seqs):
                merged[layer, b] = outs[b]
            merged[layer, seqs] = stats
            for k in ring_far:
                start(far_copy(4, k, merged.at[layer], merged_in.at[layer, k]))
            for k in ring_far[::-1]:
                far_copy(4, k, merged.at[layer], merged_in.at[layer, k]).wait_recv()
            outs, stats = combine([merged[layer], *[merged_in[layer, k] for k in ring_far]])
            for b in range(seqs):
                peak, summed = stats[:, b : b + 1], stats[:, 2 + b : 3 + b]
                top = jnp.maximum(peak, own_score[b])
                old, own = jnp.exp(peak - top), jnp.exp(own_score[b] - top)
                shared = (outs[b] * old + own * own_v[b]) / (summed * old + own)
                for r in range(group):
                    rows[b : b + 1, r * head : (r + 1) * head] = shared[r : r + 1, :]
            own_rows[layer] = rows[...].astype(BF16)
            for k in far_first:
                slot = opposite(k)
                start(block_copy(5, k, slot, own_rows.at[layer], attended.at[layer, slot]))

            weights_ready()
            branch = jnp.zeros((seqs, done.shape[1] - q_width), F32)
            for k in [0, *near_first]:
                if k:
                    block_copy(5, k, k, own_rows.at[layer], attended.at[layer, k]).wait_recv()
                piece = attended[layer, k] if k else own_rows[layer]
                branch = branch + jnp.dot(
                    piece, weights[q_columns(k), :], preferred_element_type=F32
                )
                if layer == 0:
                    done[:, q_columns(k)] = piece
                else:
                    result[0, :, q_columns(k)] = piece
            return (wide_of() + branch).astype(BF16)

        value = None
        for k in [0, *near_first]:
            copy_to(0, k, k, part.at[k], part_in.at[0, k], block_device(k, 1)).wait_recv()
            value = part_in[0, k] if value is None else value + part_in[0, k]

        def first_hidden():
            cast_hidden.wait_recv()
            return hin[1].astype(F32)

        new = after_projection(
            0, value, first_hidden, cast_mem.wait_recv, w_out_near, cast_out.wait_recv
        )
        done[:, q_width:] = new
        fetch_gain.wait()
        fetch_kv.wait()
        for k in [*far_first, 0]:
            fetch_q(k).wait()
        wide = new.astype(F32)

        def send_one(k):
            if k:
                start(copy_to(6, k, k, part.at[k], part_in.at[1, k], block_device(k, 1)))

        project(wide, lambda k: None, send_one)
        start(cast_done)
        value = part[0]
        for k in near_first:
            copy_to(6, k, k, part.at[k], part_in.at[1, k], block_device(k, 1)).wait_recv()
            value = value + part_in[1, k]

        def memory_ready():
            fetch_mem.wait()
            for k in far_first:
                regroup(k, k).wait_recv()

        new = after_projection(1, value, lambda: wide, memory_ready, w_out, fetch_out.wait)
        result[0, :, q_width:] = new
        for copy in pending:
            copy.wait_send()


def body(hidden_in, norm_gain, qkv_weight, out_weight, memory, lengths, selected):
    seqs, width = hidden_in.shape
    _, _, heads_kv, blocks_local, _, block, head = memory.shape
    heads_total = out_weight.shape[1]
    group = heads_total // (heads_kv * head)
    x_size, z_size = lax.axis_size(SEQ[0]), lax.axis_size(SEQ[1])
    sizes = (seqs, heads_kv, group, head, block, blocks_local, x_size, z_size)
    members = x_size * PAIR_Z
    far = z_size // PAIR_Z
    tile = (seqs + 1, group, head)
    hbm = pl.BlockSpec(memory_space=pltpu.HBM)
    slots = max(members, far)
    result = pl.pallas_call(
        functools.partial(kernel, sizes),
        out_shape=jax.ShapeDtypeStruct((1, seqs, heads_total + width), BF16),
        in_specs=[hbm] * 7,
        out_specs=pl.BlockSpec(memory_space=pltpu.VMEM),
        scratch_shapes=[
            pltpu.SMEM(lengths.shape, jnp.int32),
            pltpu.VMEM(selected.shape, jnp.int32),
            pltpu.VMEM((1, width), BF16),
            pltpu.VMEM((2, seqs, width), BF16),
            pltpu.VMEM(qkv_weight.shape[1:], BF16),
            pltpu.VMEM(out_weight.shape[1:], BF16),
            pltpu.VMEM(out_weight.shape[1:], BF16),
            pltpu.VMEM((members, seqs, *memory.shape[3:]), BF16),
            pltpu.VMEM((members, seqs, *memory.shape[3:]), BF16),
            pltpu.VMEM(memory.shape[1:], BF16),
            pltpu.VMEM((seqs, heads_kv, group, blocks_local * block), F32),
            pltpu.VMEM((seqs, members, group, blocks_local * block), F32),
            pltpu.VMEM((members, *tile), F32),
            pltpu.VMEM((2, members, *tile), F32),
            pltpu.VMEM((2, *tile), F32),
            pltpu.VMEM((2, far, *tile), F32),
            pltpu.VMEM((2, members, seqs, group, head), BF16),
            pltpu.VMEM((2, members, *tile), F32),
            pltpu.VMEM((2, members, *tile), F32),
            pltpu.VMEM((2, *tile), F32),
            pltpu.VMEM((2, far, *tile), F32),
            pltpu.VMEM((seqs, group * head), F32),
            pltpu.VMEM((2, seqs, group * head), BF16),
            pltpu.VMEM((2, members, seqs, group * head), BF16),
            pltpu.VMEM((seqs, heads_total + width), BF16),
            pltpu.VMEM((seqs, heads_total + width), BF16),
            pltpu.SemaphoreType.DMA((8 + members,)),
            pltpu.SemaphoreType.DMA((2, 4)),
            pltpu.SemaphoreType.REGULAR,
            pltpu.SemaphoreType.DMA((4, members)),
            pltpu.SemaphoreType.DMA((12, slots)),
            pltpu.SemaphoreType.DMA((12, slots)),
        ],
        compiler_params=pltpu.CompilerParams(
            collective_id=0, has_side_effects=True, vmem_limit_bytes=VMEM_BYTES
        ),
        name="decode",
    )(lengths, hidden_in, norm_gain, selected, qkv_weight, out_weight, memory)
    return result[:, :, heads_total:], result[:, :, :heads_total]


def solution(mesh):
    z_size = mesh.shape["seq"] // RING_X
    finer = Mesh(
        mesh.devices.reshape(mesh.shape["groups"], RING_X, z_size, mesh.shape["section"]),
        ("groups", *SEQ, "section"),
    )
    in_specs = (
        P("groups", SEQ),
        P("section", SEQ),
        P("section", SEQ, None),
        P("section", None, SEQ),
        P("section", "groups", None, SEQ, None, None, None),
        P("groups"),
        P("groups", None, None),
    )
    out_specs = (P("section", "groups", SEQ), P("section", "groups", None))
    return jax.shard_map(body, mesh=finer, in_specs=in_specs, out_specs=out_specs, check_vma=False)
```

```python
import functools

import jax
import jax.numpy as jnp
from jax import lax
from jax.experimental import pallas as pl
from jax.experimental.pallas import tpu as pltpu
from jax.sharding import Mesh
from jax.sharding import PartitionSpec as P

MESH = pl.DeviceIdType.MESH
EPSILON = 1e-05
FLOOR = -1e30
RING_X = 4
PAIR_Z = 2
SEQ = ("seq_0", "seq_1")
F32, BF16 = jnp.float32, jnp.bfloat16
VMEM_BYTES = 64000000


def kernel(
    sizes,
    lengths_hbm,
    hidden_hbm,
    gain_hbm,
    selected_hbm,
    qkv_hbm,
    out_hbm,
    memory_hbm,
    result,
    lengths,
    selected,
    gain,
    hin,
    w_in,
    w_out,
    w_out_near,
    mem_stage,
    mem_block,
    mem_near,
    live,
    live_block,
    part,
    part_in,
    total,
    total_in,
    query,
    local,
    local_in,
    merged,
    merged_in,
    rows,
    own_rows,
    attended,
    done,
    done_in,
    fetch_sem,
    cast_sem,
    ready_sem,
    group_sem,
    send,
    recv,
):
    seqs, heads_kv, group, head, block, blocks_local, x_size, z_size = sizes
    lanes = group * head
    q_width = heads_kv * lanes
    kv_width = heads_kv * head
    tokens = blocks_local * block
    far_size = z_size // PAIR_Z
    offsets = [(dx, dz) for dx in range(x_size) for dz in range(PAIR_Z)]
    hops = [min(dx, x_size - dx) + dz for dx, dz in offsets]
    near_first = sorted(range(1, len(offsets)), key=lambda k: hops[k])
    far_first = near_first[::-1]
    ring_far = sorted(range(1, far_size), key=lambda k: -min(k, far_size - k))

    x = lax.axis_index(SEQ[0])
    z = lax.axis_index(SEQ[1])
    section = lax.axis_index("section")
    pair = lax.rem(z, PAIR_Z)
    base_z = z - pair
    first_block = (x * z_size + z) * blocks_local
    scale = head ** (-0.5)
    model_width = hin.shape[2] * x_size * z_size

    def in_block(k):
        dx, dz = offsets[k]
        return lax.rem(x + dx, x_size), lax.rem(pair + dz, PAIR_Z)

    def kv_of(k):
        bx, bz = in_block(k)
        return bx * PAIR_Z + bz

    def block_device(k, core):
        bx, bz = in_block(k)
        return {SEQ[0]: bx, SEQ[1]: base_z + bz, "section": core}

    def far_device(k):
        return {SEQ[1]: lax.rem(z + k * PAIR_Z, z_size)}

    def opposite(k):
        dx, dz = offsets[k]
        return offsets.index(((x_size - dx) % x_size, dz))

    barrier = pltpu.get_barrier_semaphore()

    def greet(device):
        pl.semaphore_signal(barrier, inc=1, device_id=device, device_id_type=MESH)

    def copy_to(stage, k, slot, source, target, device):
        return pltpu.make_async_remote_copy(
            src_ref=source,
            dst_ref=target,
            send_sem=send.at[stage, k],
            recv_sem=recv.at[stage, slot],
            device_id=device,
            device_id_type=MESH,
        )

    def cast(number, source, target, core):
        return pltpu.make_async_remote_copy(
            src_ref=source,
            dst_ref=target,
            send_sem=cast_sem.at[0, number],
            recv_sem=cast_sem.at[1, number],
            device_id={"section": core},
            device_id_type=MESH,
        )

    def stage_memory(k):
        return pltpu.make_async_remote_copy(
            src_ref=memory_hbm.at[0, :, kv_of(k)],
            dst_ref=mem_stage.at[k],
            send_sem=group_sem.at[0, k],
            recv_sem=group_sem.at[1, k],
            device_id={"section": 0},
            device_id_type=MESH,
        )

    def regroup(k, slot, piece=()):
        return pltpu.make_async_remote_copy(
            src_ref=mem_stage.at[(k, *piece)],
            dst_ref=mem_block.at[(slot, *piece)],
            send_sem=group_sem.at[2, k],
            recv_sem=group_sem.at[3, slot],
            device_id=block_device(k, 1),
            device_id_type=MESH,
        )

    cast_hidden = cast(0, hidden_hbm, hin.at[1], 1)
    cast_mem = cast(1, memory_hbm.at[0], mem_near, 1)
    cast_out = cast(2, out_hbm.at[0], w_out_near, 1)
    cast_done = cast(3, done, done_in, 0)

    fetch_gain = pltpu.make_async_copy(gain_hbm, gain, fetch_sem.at[0])
    fetch_hidden = pltpu.make_async_copy(hidden_hbm, hin.at[0], fetch_sem.at[1])
    fetch_kv = pltpu.make_async_copy(
        qkv_hbm.at[0, :, pl.ds(q_width, 2 * kv_width)],
        w_in.at[:, pl.ds(q_width, 2 * kv_width)],
        fetch_sem.at[2],
    )

    def q_columns(k):
        return pl.ds(pl.multiple_of(kv_of(k) * lanes, lanes), lanes)

    def fetch_q(k):
        return pltpu.make_async_copy(
            qkv_hbm.at[0, :, q_columns(k)], w_in.at[:, q_columns(k)], fetch_sem.at[8 + k]
        )

    fetch_selected = pltpu.make_async_copy(selected_hbm, selected, fetch_sem.at[3])
    fetch_lengths = pltpu.make_async_copy(lengths_hbm, lengths, fetch_sem.at[4])
    fetch_mem = pltpu.make_async_copy(
        memory_hbm.at[0, :, kv_of(0)], mem_block.at[0], fetch_sem.at[5]
    )
    fetch_out = pltpu.make_async_copy(out_hbm.at[0], w_out, fetch_sem.at[6])

    @pl.when(section == 0)
    def _():
        greet({"section": 1})

    @pl.when(section == 1)
    def _():
        for k in [*far_first, 0]:
            greet(block_device(k, 0))
        for k in ring_far:
            greet(far_device(k))
        for k in far_first:
            greet(block_device(k, 1))

    fetch_gain.start()

    @pl.when(section == 0)
    def _():
        fetch_hidden.start()

    fetch_kv.start()
    for k in [*far_first, 0]:
        fetch_q(k).start()

    def project(wide, ready, send_one):
        normed = (wide * gain[...].astype(F32)).astype(BF16)
        squares = wide * wide
        for k in [*far_first, 0]:
            g = kv_of(k)
            at_k = pl.multiple_of(q_width + g * head, head)
            at_v = pl.multiple_of(q_width + kv_width + g * head, head)
            ready(k)
            qs = jnp.dot(normed, w_in[:, q_columns(k)], preferred_element_type=F32)
            ks = jnp.dot(normed, w_in[:, pl.ds(at_k, head)], preferred_element_type=F32)
            vs = jnp.dot(normed, w_in[:, pl.ds(at_v, head)], preferred_element_type=F32)
            for b in range(seqs):
                for r in range(group):
                    part[k, b, r : r + 1, :] = qs[b : b + 1, r * head : (r + 1) * head]
            part[k, seqs, 0:2, :] = ks
            part[k, seqs, 2:4, :] = vs
            part[k, seqs, 4:6, :] = squares
            part[k, seqs, 6:8, :] = jnp.zeros((2, head), F32)
            send_one(k)

    @pl.when(section == 0)
    def _():
        fetch_gain.wait()
        fetch_hidden.wait()
        fetch_kv.wait()
        sent = []

        def send_one(k):
            if not sent:
                pl.semaphore_wait(barrier, len(offsets))
                pl.semaphore_signal(
                    ready_sem, inc=1, device_id={"section": 1}, device_id_type=MESH
                )
            copy = copy_to(0, k, k, part.at[k], part_in.at[0, k], block_device(k, 1))
            copy.start()
            sent.append(copy)

        project(hin[0].astype(F32), lambda k: fetch_q(k).wait(), send_one)
        cast_hidden.start()
        cast_mem.start()
        cast_out.start()
        for k in far_first:
            stage_memory(k).wait_recv()
            sent.append(regroup(k, opposite(k)))
        for b in range(seqs):
            for n in range(blocks_local):
                for k in far_first:
                    regroup(k, opposite(k), (b, n)).start()
        for copy in [*sent, cast_hidden, cast_mem, cast_out]:
            copy.wait_send()
        cast_done.wait_recv()
        result[0] = done_in[...]

    @pl.when(section == 1)
    def _():
        pending = []

        def start(copy):
            copy.start()
            pending.append(copy)

        fetch_selected.start()
        fetch_lengths.start()
        fetch_mem.start()
        fetch_out.start()

        fetch_selected.wait()
        fetch_lengths.wait()
        lane = lax.broadcasted_iota(jnp.int32, (heads_kv, tokens), 1)
        for b in range(seqs):
            chosen_ids = selected[b]
            lane_block = first_block + lane // block
            hit = jnp.zeros((heads_kv, tokens), F32)
            for s in range(selected.shape[2]):
                hit = jnp.where(chosen_ids[:, s : s + 1] == lane_block, 1.0, hit)
            hit = jnp.where(first_block * block + lane < lengths[b], hit, 0.0)
            for g in range(heads_kv):
                live[b, g] = jnp.broadcast_to(hit[g : g + 1, :], (group, tokens))

        pl.semaphore_wait(ready_sem, 1)
        for k in far_first:
            start(stage_memory(k))

        row = lax.broadcasted_iota(jnp.int32, (len(offsets), tokens), 0)
        row_lane = lax.broadcasted_iota(jnp.int32, (len(offsets), tokens), 1)
        row_first = jnp.zeros((len(offsets), tokens), jnp.int32)
        for k in range(len(offsets)):
            bx, bz = in_block(k)
            row_first = jnp.where(
                row == k, (bx * z_size + base_z + bz) * blocks_local, row_first
            )
        for b in range(seqs):
            chosen_ids = selected[b, pl.ds(kv_of(0), 1), :]
            hit = jnp.zeros((len(offsets), tokens), F32)
            for s in range(selected.shape[2]):
                hit = jnp.where(
                    chosen_ids[:, s : s + 1] == row_first + row_lane // block, 1.0, hit
                )
            hit = jnp.where(row_first * block + row_lane < lengths[b], hit, 0.0)
            for k in range(len(offsets)):
                live_block[b, k] = jnp.broadcast_to(hit[k : k + 1, :], (group, tokens))
        stat_lane = lax.broadcasted_iota(jnp.int32, (group, head), 1)
        def score_of(q, keys, mask):
            score = lax.dot_general(
                q, keys, (((1,), (1,)), ((), ())), preferred_element_type=F32
            )
            return jnp.where(mask, score * scale, FLOOR)

        def mix(weight, values):
            high = weight.astype(BF16)
            low = (weight - high.astype(F32)).astype(BF16)
            mixed = jnp.dot(
                jnp.concatenate([high, low], axis=0), values, preferred_element_type=F32
            )
            return mixed[:group] + mixed[group:]

        def stats_of(peaks, sums):
            stats = jnp.where(stat_lane < 3, sums[0], sums[1])
            stats = jnp.where(stat_lane < 2, peaks[1], stats)
            return jnp.where(stat_lane < 1, peaks[0], stats)

        def attend(layer, ks, memory):
            pairs = [(k, b) for k in ks for b in range(seqs)]
            heads = [kv_of(k) for k, b in pairs]
            masks = [live[b, g] > 0.5 for (k, b), g in zip(pairs, heads)]
            scores = [
                score_of(query[layer, k, b], memory[b, g, :, 0].reshape(tokens, head), mask)
                for (k, b), g, mask in zip(pairs, heads, masks)
            ]
            peaks = [jnp.max(score, axis=1, keepdims=True) for score in scores]
            weights = [
                jnp.where(mask, jnp.exp(score - peak), 0.0)
                for score, peak, mask in zip(scores, peaks, masks)
            ]
            sums = [jnp.sum(weight, axis=1, keepdims=True) for weight in weights]
            for (k, b), g, weight in zip(pairs, heads, weights):
                local[layer, k, b] = mix(weight, memory[b, g, :, 1].reshape(tokens, head))
            for n, k in enumerate(ks):
                at = slice(n * seqs, (n + 1) * seqs)
                local[layer, k, seqs] = stats_of(peaks[at], sums[at])

        def attend_block(layer):
            members = range(len(offsets))
            outs, peaks, sums = [], [], []
            for b in range(seqs):
                masks = [live_block[b, k] > 0.5 for k in members]
                scores = [
                    score_of(
                        query[layer, 0, b], mem_block[k, b, :, 0].reshape(tokens, head), masks[k]
                    )
                    for k in members
                ]
                highest = scores[0]
                for score in scores[1:]:
                    highest = jnp.maximum(highest, score)
                peak = jnp.max(highest, axis=1, keepdims=True)
                out = jnp.zeros((group, head), F32)
                total_weight = jnp.zeros((group, tokens), F32)
                for k in members:
                    weight = jnp.where(masks[k], jnp.exp(scores[k] - peak), 0.0)
                    total_weight = total_weight + weight
                    out = out + mix(weight, mem_block[k, b, :, 1].reshape(tokens, head))
                outs.append(out)
                peaks.append(peak)
                sums.append(jnp.sum(total_weight, axis=1, keepdims=True))
            return outs, stats_of(peaks, sums)

        def combine(parts):
            top = parts[0][seqs]
            for p in parts[1:]:
                top = jnp.maximum(top, p[seqs])
            sums = jnp.zeros((group, head), F32)
            outs = [jnp.zeros((group, head), F32) for _ in range(seqs)]
            for p in parts:
                factor = jnp.where(stat_lane < 2, jnp.exp(jnp.minimum(p[seqs] - top, 0.0)), 0.0)
                wides = [
                    jnp.broadcast_to(factor[:, b : b + 1], (group, head)) for b in range(seqs)
                ]
                sums = sums + p[seqs] * jnp.where(stat_lane < 3, wides[0], wides[1])
                outs = [outs[b] + p[b] * wides[b] for b in range(seqs)]
            return outs, jnp.where(stat_lane < 2, top, sums)

        def after_projection(layer, value, wide_of, memory_ready, weights, weights_ready):
            stage = 6 * layer
            total[layer] = value
            if layer == 0:
                pl.semaphore_wait(barrier, len(ring_far) + len(far_first) + 1)

            def far_copy(n, k, source, target):
                return copy_to(stage + n, k, k, source, target, far_device(k))

            def block_copy(n, k, slot, source, target):
                return copy_to(stage + n, k, slot, source, target, block_device(k, 1))

            for k in ring_far:
                start(far_copy(1, k, total.at[layer], total_in.at[layer, k]))
            for k in ring_far[::-1]:
                far_copy(1, k, total.at[layer], total_in.at[layer, k]).wait_recv()
                value = value + total_in[layer, k]

            own_q, own_k, own_v = [], [], []
            for b in range(seqs):
                mean = jnp.sum(value[seqs, 4 + b : 5 + b, :], axis=1, keepdims=True) / model_width
                inverse = lax.rsqrt(mean + EPSILON)
                q = (value[b] * inverse).astype(BF16)
                query[layer, 0, b] = q
                own_q.append(q.astype(F32))
                own_k.append((value[seqs, b : b + 1, :] * inverse).astype(BF16).astype(F32))
                own_v.append((value[seqs, 2 + b : 3 + b, :] * inverse).astype(BF16).astype(F32))
            if layer == 0:
                for k in far_first:
                    slot = opposite(k)
                    start(block_copy(2, k, slot, query.at[layer, 0], query.at[layer, slot]))
            own_score = [
                jnp.sum(own_q[b] * own_k[b], axis=1, keepdims=True) * scale for b in range(seqs)
            ]

            memory_ready()
            if layer == 0:
                attend(layer, [0], mem_near)
                for distance in sorted({hops[k] for k in near_first}):
                    batch = [k for k in near_first if hops[k] == distance]
                    for k in batch:
                        block_copy(2, k, k, query.at[layer, 0], query.at[layer, k]).wait_recv()
                    attend(layer, batch, mem_near)
                    for k in batch:
                        start(block_copy(3, k, k, local.at[layer, k], local_in.at[layer, k]))
                for k in near_first:
                    block_copy(3, k, k, local.at[layer, k], local_in.at[layer, k]).wait_recv()
                outs, stats = combine([local[layer, 0], *[local_in[layer, k] for k in near_first]])
            else:
                outs, stats = attend_block(layer)
            for b in range(seqs):
                merged[layer, b] = outs[b]
            merged[layer, seqs] = stats
            for k in ring_far:
                start(far_copy(4, k, merged.at[layer], merged_in.at[layer, k]))
            for k in ring_far[::-1]:
                far_copy(4, k, merged.at[layer], merged_in.at[layer, k]).wait_recv()
            outs, stats = combine([merged[layer], *[merged_in[layer, k] for k in ring_far]])
            for b in range(seqs):
                peak, summed = stats[:, b : b + 1], stats[:, 2 + b : 3 + b]
                top = jnp.maximum(peak, own_score[b])
                old, own = jnp.exp(peak - top), jnp.exp(own_score[b] - top)
                shared = (outs[b] * old + own * own_v[b]) / (summed * old + own)
                for r in range(group):
                    rows[b : b + 1, r * head : (r + 1) * head] = shared[r : r + 1, :]
            own_rows[layer] = rows[...].astype(BF16)
            for k in far_first:
                slot = opposite(k)
                start(block_copy(5, k, slot, own_rows.at[layer], attended.at[layer, slot]))

            weights_ready()
            branch = jnp.zeros((seqs, done.shape[1] - q_width), F32)
            for k in [0, *near_first]:
                if k:
                    block_copy(5, k, k, own_rows.at[layer], attended.at[layer, k]).wait_recv()
                piece = attended[layer, k] if k else own_rows[layer]
                branch = branch + jnp.dot(
                    piece, weights[q_columns(k), :], preferred_element_type=F32
                )
                if layer == 0:
                    done[:, q_columns(k)] = piece
                else:
                    result[0, :, q_columns(k)] = piece
            return (wide_of() + branch).astype(BF16)

        value = None
        for k in [0, *near_first]:
            copy_to(0, k, k, part.at[k], part_in.at[0, k], block_device(k, 1)).wait_recv()
            value = part_in[0, k] if value is None else value + part_in[0, k]

        def first_hidden():
            cast_hidden.wait_recv()
            return hin[1].astype(F32)

        new = after_projection(
            0, value, first_hidden, cast_mem.wait_recv, w_out_near, cast_out.wait_recv
        )
        done[:, q_width:] = new
        fetch_gain.wait()
        fetch_kv.wait()
        for k in [*far_first, 0]:
            fetch_q(k).wait()
        wide = new.astype(F32)

        def send_one(k):
            if k:
                start(copy_to(6, k, k, part.at[k], part_in.at[1, k], block_device(k, 1)))

        project(wide, lambda k: None, send_one)
        start(cast_done)
        value = part[0]
        for k in near_first:
            copy_to(6, k, k, part.at[k], part_in.at[1, k], block_device(k, 1)).wait_recv()
            value = value + part_in[1, k]

        def memory_ready():
            fetch_mem.wait()
            for k in far_first:
                regroup(k, k).wait_recv()

        new = after_projection(1, value, lambda: wide, memory_ready, w_out, fetch_out.wait)
        result[0, :, q_width:] = new
        for copy in pending:
            copy.wait_send()


def body(hidden_in, norm_gain, qkv_weight, out_weight, memory, lengths, selected):
    seqs, width = hidden_in.shape
    _, _, heads_kv, blocks_local, _, block, head = memory.shape
    heads_total = out_weight.shape[1]
    group = heads_total // (heads_kv * head)
    x_size, z_size = lax.axis_size(SEQ[0]), lax.axis_size(SEQ[1])
    sizes = (seqs, heads_kv, group, head, block, blocks_local, x_size, z_size)
    members = x_size * PAIR_Z
    far = z_size // PAIR_Z
    tile = (seqs + 1, group, head)
    hbm = pl.BlockSpec(memory_space=pltpu.HBM)
    slots = max(members, far)
    result = pl.pallas_call(
        functools.partial(kernel, sizes),
        out_shape=jax.ShapeDtypeStruct((1, seqs, heads_total + width), BF16),
        in_specs=[hbm] * 7,
        out_specs=pl.BlockSpec(memory_space=pltpu.VMEM),
        scratch_shapes=[
            pltpu.SMEM(lengths.shape, jnp.int32),
            pltpu.VMEM(selected.shape, jnp.int32),
            pltpu.VMEM((1, width), BF16),
            pltpu.VMEM((2, seqs, width), BF16),
            pltpu.VMEM(qkv_weight.shape[1:], BF16),
            pltpu.VMEM(out_weight.shape[1:], BF16),
            pltpu.VMEM(out_weight.shape[1:], BF16),
            pltpu.VMEM((members, seqs, *memory.shape[3:]), BF16),
            pltpu.VMEM((members, seqs, *memory.shape[3:]), BF16),
            pltpu.VMEM(memory.shape[1:], BF16),
            pltpu.VMEM((seqs, heads_kv, group, blocks_local * block), F32),
            pltpu.VMEM((seqs, members, group, blocks_local * block), F32),
            pltpu.VMEM((members, *tile), F32),
            pltpu.VMEM((2, members, *tile), F32),
            pltpu.VMEM((2, *tile), F32),
            pltpu.VMEM((2, far, *tile), F32),
            pltpu.VMEM((2, members, seqs, group, head), BF16),
            pltpu.VMEM((2, members, *tile), F32),
            pltpu.VMEM((2, members, *tile), F32),
            pltpu.VMEM((2, *tile), F32),
            pltpu.VMEM((2, far, *tile), F32),
            pltpu.VMEM((seqs, group * head), F32),
            pltpu.VMEM((2, seqs, group * head), BF16),
            pltpu.VMEM((2, members, seqs, group * head), BF16),
            pltpu.VMEM((seqs, heads_total + width), BF16),
            pltpu.VMEM((seqs, heads_total + width), BF16),
            pltpu.SemaphoreType.DMA((8 + members,)),
            pltpu.SemaphoreType.DMA((2, 4)),
            pltpu.SemaphoreType.REGULAR,
            pltpu.SemaphoreType.DMA((4, members)),
            pltpu.SemaphoreType.DMA((12, slots)),
            pltpu.SemaphoreType.DMA((12, slots)),
        ],
        compiler_params=pltpu.CompilerParams(
            collective_id=0, has_side_effects=True, vmem_limit_bytes=VMEM_BYTES
        ),
        name="decode",
    )(lengths, hidden_in, norm_gain, selected, qkv_weight, out_weight, memory)
    return result[:, :, heads_total:], result[:, :, :heads_total]


def solution(mesh):
    z_size = mesh.shape["seq"] // RING_X
    finer = Mesh(
        mesh.devices.reshape(mesh.shape["groups"], RING_X, z_size, mesh.shape["section"]),
        ("groups", *SEQ, "section"),
    )
    in_specs = (
        P("groups", SEQ),
        P("section", SEQ),
        P("section", SEQ, None),
        P("section", None, SEQ),
        P("section", "groups", None, SEQ, None, None, None),
        P("groups"),
        P("groups", None, None),
    )
    out_specs = (P("section", "groups", SEQ), P("section", "groups", None))
    return jax.shard_map(body, mesh=finer, in_specs=in_specs, out_specs=out_specs, check_vma=False)
```

```python
import functools

import jax
import jax.numpy as jnp
from jax import lax
from jax.experimental import pallas as pl
from jax.experimental.pallas import tpu as pltpu
from jax.sharding import Mesh
from jax.sharding import PartitionSpec as P

MESH = pl.DeviceIdType.MESH
EPSILON = 1e-05
FLOOR = -1e30
RING_X = 4
PAIR_Z = 2
SEQ = ("seq_0", "seq_1")
F32, BF16 = jnp.float32, jnp.bfloat16
VMEM_BYTES = 64000000


def kernel(
    sizes,
    lengths_hbm,
    hidden_hbm,
    gain_hbm,
    selected_hbm,
    qkv_hbm,
    out_hbm,
    memory_hbm,
    result,
    lengths,
    selected,
    gain,
    hin,
    w_in,
    w_out,
    w_out_near,
    mem_stage,
    mem_block,
    mem_near,
    live,
    live_block,
    part,
    part_in,
    total,
    total_in,
    query,
    local,
    local_in,
    merged,
    merged_in,
    rows,
    own_rows,
    attended,
    done,
    done_in,
    fetch_sem,
    cast_sem,
    ready_sem,
    group_sem,
    send,
    recv,
):
    seqs, heads_kv, group, head, block, blocks_local, x_size, z_size = sizes
    lanes = group * head
    q_width = heads_kv * lanes
    kv_width = heads_kv * head
    tokens = blocks_local * block
    far_size = z_size // PAIR_Z
    offsets = [(dx, dz) for dx in range(x_size) for dz in range(PAIR_Z)]
    hops = [min(dx, x_size - dx) + dz for dx, dz in offsets]
    near_first = sorted(range(1, len(offsets)), key=lambda k: hops[k])
    far_first = near_first[::-1]
    ring_far = sorted(range(1, far_size), key=lambda k: -min(k, far_size - k))

    x = lax.axis_index(SEQ[0])
    z = lax.axis_index(SEQ[1])
    section = lax.axis_index("section")
    pair = lax.rem(z, PAIR_Z)
    base_z = z - pair
    first_block = (x * z_size + z) * blocks_local
    scale = head ** (-0.5)
    model_width = hin.shape[2] * x_size * z_size

    def in_block(k):
        dx, dz = offsets[k]
        return lax.rem(x + dx, x_size), lax.rem(pair + dz, PAIR_Z)

    def kv_of(k):
        bx, bz = in_block(k)
        return bx * PAIR_Z + bz

    def block_device(k, core):
        bx, bz = in_block(k)
        return {SEQ[0]: bx, SEQ[1]: base_z + bz, "section": core}

    def far_device(k):
        return {SEQ[1]: lax.rem(z + k * PAIR_Z, z_size)}

    def opposite(k):
        dx, dz = offsets[k]
        return offsets.index(((x_size - dx) % x_size, dz))

    barrier = pltpu.get_barrier_semaphore()

    def greet(device):
        pl.semaphore_signal(barrier, inc=1, device_id=device, device_id_type=MESH)

    def copy_to(stage, k, slot, source, target, device):
        return pltpu.make_async_remote_copy(
            src_ref=source,
            dst_ref=target,
            send_sem=send.at[stage, k],
            recv_sem=recv.at[stage, slot],
            device_id=device,
            device_id_type=MESH,
        )

    def cast(number, source, target, core):
        return pltpu.make_async_remote_copy(
            src_ref=source,
            dst_ref=target,
            send_sem=cast_sem.at[0, number],
            recv_sem=cast_sem.at[1, number],
            device_id={"section": core},
            device_id_type=MESH,
        )

    def stage_memory(k):
        return pltpu.make_async_remote_copy(
            src_ref=memory_hbm.at[0, :, kv_of(k)],
            dst_ref=mem_stage.at[k],
            send_sem=group_sem.at[0, k],
            recv_sem=group_sem.at[1, k],
            device_id={"section": 0},
            device_id_type=MESH,
        )

    def regroup(k, slot, piece=()):
        return pltpu.make_async_remote_copy(
            src_ref=mem_stage.at[(k, *piece)],
            dst_ref=mem_block.at[(slot, *piece)],
            send_sem=group_sem.at[2, k],
            recv_sem=group_sem.at[3, slot],
            device_id=block_device(k, 1),
            device_id_type=MESH,
        )

    cast_hidden = cast(0, hidden_hbm, hin.at[1], 1)
    cast_mem = cast(1, memory_hbm.at[0], mem_near, 1)
    cast_out = cast(2, out_hbm.at[0], w_out_near, 1)
    cast_done = cast(3, done, done_in, 0)

    fetch_gain = pltpu.make_async_copy(gain_hbm, gain, fetch_sem.at[0])
    fetch_hidden = pltpu.make_async_copy(hidden_hbm, hin.at[0], fetch_sem.at[1])
    fetch_kv = pltpu.make_async_copy(
        qkv_hbm.at[0, :, pl.ds(q_width, 2 * kv_width)],
        w_in.at[:, pl.ds(q_width, 2 * kv_width)],
        fetch_sem.at[2],
    )

    def q_columns(k):
        return pl.ds(pl.multiple_of(kv_of(k) * lanes, lanes), lanes)

    def fetch_q(k):
        return pltpu.make_async_copy(
            qkv_hbm.at[0, :, q_columns(k)], w_in.at[:, q_columns(k)], fetch_sem.at[8 + k]
        )

    fetch_selected = pltpu.make_async_copy(selected_hbm, selected, fetch_sem.at[3])
    fetch_lengths = pltpu.make_async_copy(lengths_hbm, lengths, fetch_sem.at[4])
    fetch_mem = pltpu.make_async_copy(
        memory_hbm.at[0, :, kv_of(0)], mem_block.at[0], fetch_sem.at[5]
    )
    fetch_out = pltpu.make_async_copy(out_hbm.at[0], w_out, fetch_sem.at[6])

    @pl.when(section == 0)
    def _():
        greet({"section": 1})

    @pl.when(section == 1)
    def _():
        for k in [*far_first, 0]:
            greet(block_device(k, 0))
        for k in ring_far:
            greet(far_device(k))
        for k in far_first:
            greet(block_device(k, 1))

    fetch_gain.start()

    @pl.when(section == 0)
    def _():
        fetch_hidden.start()

    fetch_kv.start()
    for k in [*far_first, 0]:
        fetch_q(k).start()

    def project(wide, ready, send_one):
        normed = (wide * gain[...].astype(F32)).astype(BF16)
        squares = jnp.broadcast_to(jnp.sum(wide * wide, axis=1, keepdims=True), wide.shape)
        for k in [*far_first, 0]:
            g = kv_of(k)
            at_k = pl.multiple_of(q_width + g * head, head)
            at_v = pl.multiple_of(q_width + kv_width + g * head, head)
            ready(k)
            qs = jnp.dot(normed, w_in[:, q_columns(k)], preferred_element_type=F32)
            ks = jnp.dot(normed, w_in[:, pl.ds(at_k, head)], preferred_element_type=F32)
            vs = jnp.dot(normed, w_in[:, pl.ds(at_v, head)], preferred_element_type=F32)
            for b in range(seqs):
                for r in range(group):
                    part[k, b, r : r + 1, :] = qs[b : b + 1, r * head : (r + 1) * head]
            part[k, seqs, 0:2, :] = ks
            part[k, seqs, 2:4, :] = vs
            part[k, seqs, 4:6, :] = squares
            part[k, seqs, 6:8, :] = jnp.zeros((2, head), F32)
            send_one(k)

    @pl.when(section == 0)
    def _():
        fetch_gain.wait()
        fetch_hidden.wait()
        fetch_kv.wait()
        sent = []

        def send_one(k):
            if not sent:
                pl.semaphore_wait(barrier, len(offsets))
                pl.semaphore_signal(
                    ready_sem, inc=1, device_id={"section": 1}, device_id_type=MESH
                )
            copy = copy_to(0, k, k, part.at[k], part_in.at[0, k], block_device(k, 1))
            copy.start()
            sent.append(copy)

        project(hin[0].astype(F32), lambda k: fetch_q(k).wait(), send_one)
        cast_hidden.start()
        cast_mem.start()
        cast_out.start()
        for k in far_first:
            stage_memory(k).wait_recv()
            sent.append(regroup(k, opposite(k)))
        for b in range(seqs):
            for n in range(blocks_local):
                for half in range(2):
                    for k in far_first:
                        regroup(k, opposite(k), (b, n, half)).start()
        for copy in [*sent, cast_hidden, cast_mem, cast_out]:
            copy.wait_send()
        cast_done.wait_recv()
        result[0] = done_in[...]

    @pl.when(section == 1)
    def _():
        pending = []

        def start(copy):
            copy.start()
            pending.append(copy)

        fetch_selected.start()
        fetch_lengths.start()
        fetch_mem.start()
        fetch_out.start()

        fetch_selected.wait()
        fetch_lengths.wait()
        lane = lax.broadcasted_iota(jnp.int32, (heads_kv, tokens), 1)
        for b in range(seqs):
            chosen_ids = selected[b]
            lane_block = first_block + lane // block
            hit = jnp.zeros((heads_kv, tokens), F32)
            for s in range(selected.shape[2]):
                hit = jnp.where(chosen_ids[:, s : s + 1] == lane_block, 1.0, hit)
            hit = jnp.where(first_block * block + lane < lengths[b], hit, 0.0)
            for g in range(heads_kv):
                live[b, g] = jnp.broadcast_to(hit[g : g + 1, :], (group, tokens))

        pl.semaphore_wait(ready_sem, 1)
        for k in far_first:
            start(stage_memory(k))

        row = lax.broadcasted_iota(jnp.int32, (len(offsets), tokens), 0)
        row_lane = lax.broadcasted_iota(jnp.int32, (len(offsets), tokens), 1)
        row_first = jnp.zeros((len(offsets), tokens), jnp.int32)
        for k in range(len(offsets)):
            bx, bz = in_block(k)
            row_first = jnp.where(
                row == k, (bx * z_size + base_z + bz) * blocks_local, row_first
            )
        for b in range(seqs):
            chosen_ids = selected[b, pl.ds(kv_of(0), 1), :]
            hit = jnp.zeros((len(offsets), tokens), F32)
            for s in range(selected.shape[2]):
                hit = jnp.where(
                    chosen_ids[:, s : s + 1] == row_first + row_lane // block, 1.0, hit
                )
            hit = jnp.where(row_first * block + row_lane < lengths[b], hit, 0.0)
            for k in range(len(offsets)):
                live_block[b, k] = jnp.broadcast_to(hit[k : k + 1, :], (group, tokens))
        stat_lane = lax.broadcasted_iota(jnp.int32, (group, head), 1)
        def score_of(q, keys, mask):
            score = lax.dot_general(
                q, keys, (((1,), (1,)), ((), ())), preferred_element_type=F32
            )
            return jnp.where(mask, score * scale, FLOOR)

        def mix(weight, values):
            high = weight.astype(BF16)
            low = (weight - high.astype(F32)).astype(BF16)
            mixed = jnp.dot(
                jnp.concatenate([high, low], axis=0), values, preferred_element_type=F32
            )
            return mixed[:group] + mixed[group:]

        def stats_of(peaks, sums):
            stats = jnp.where(stat_lane < 3, sums[0], sums[1])
            stats = jnp.where(stat_lane < 2, peaks[1], stats)
            return jnp.where(stat_lane < 1, peaks[0], stats)

        def attend(layer, ks, memory):
            pairs = [(k, b) for k in ks for b in range(seqs)]
            heads = [kv_of(k) for k, b in pairs]
            masks = [live[b, g] > 0.5 for (k, b), g in zip(pairs, heads)]
            scores = [
                score_of(query[layer, k, b], memory[b, g, :, 0].reshape(tokens, head), mask)
                for (k, b), g, mask in zip(pairs, heads, masks)
            ]
            peaks = [jnp.max(score, axis=1, keepdims=True) for score in scores]
            weights = [
                jnp.where(mask, jnp.exp(score - peak), 0.0)
                for score, peak, mask in zip(scores, peaks, masks)
            ]
            sums = [jnp.sum(weight, axis=1, keepdims=True) for weight in weights]
            for (k, b), g, weight in zip(pairs, heads, weights):
                local[layer, k, b] = mix(weight, memory[b, g, :, 1].reshape(tokens, head))
            for n, k in enumerate(ks):
                at = slice(n * seqs, (n + 1) * seqs)
                local[layer, k, seqs] = stats_of(peaks[at], sums[at])

        def attend_block(layer):
            members = range(len(offsets))
            outs, peaks, sums = [], [], []
            for b in range(seqs):
                masks = [live_block[b, k] > 0.5 for k in members]
                scores = [
                    score_of(
                        query[layer, 0, b], mem_block[k, b, :, 0].reshape(tokens, head), masks[k]
                    )
                    for k in members
                ]
                highest = scores[0]
                for score in scores[1:]:
                    highest = jnp.maximum(highest, score)
                peak = jnp.max(highest, axis=1, keepdims=True)
                out = jnp.zeros((group, head), F32)
                total_weight = jnp.zeros((group, tokens), F32)
                for k in members:
                    weight = jnp.where(masks[k], jnp.exp(scores[k] - peak), 0.0)
                    total_weight = total_weight + weight
                    out = out + mix(weight, mem_block[k, b, :, 1].reshape(tokens, head))
                outs.append(out)
                peaks.append(peak)
                sums.append(jnp.sum(total_weight, axis=1, keepdims=True))
            return outs, stats_of(peaks, sums)

        def combine(parts):
            top = parts[0][seqs]
            for p in parts[1:]:
                top = jnp.maximum(top, p[seqs])
            sums = jnp.zeros((group, head), F32)
            outs = [jnp.zeros((group, head), F32) for _ in range(seqs)]
            for p in parts:
                factor = jnp.where(stat_lane < 2, jnp.exp(jnp.minimum(p[seqs] - top, 0.0)), 0.0)
                wides = [
                    jnp.broadcast_to(factor[:, b : b + 1], (group, head)) for b in range(seqs)
                ]
                sums = sums + p[seqs] * jnp.where(stat_lane < 3, wides[0], wides[1])
                outs = [outs[b] + p[b] * wides[b] for b in range(seqs)]
            return outs, jnp.where(stat_lane < 2, top, sums)

        def after_projection(layer, value, wide_of, memory_ready, weights, weights_ready):
            stage = 6 * layer
            total[layer] = value
            if layer == 0:
                pl.semaphore_wait(barrier, len(ring_far) + len(far_first) + 1)

            def far_copy(n, k, source, target):
                return copy_to(stage + n, k, k, source, target, far_device(k))

            def block_copy(n, k, slot, source, target):
                return copy_to(stage + n, k, slot, source, target, block_device(k, 1))

            for k in ring_far:
                start(far_copy(1, k, total.at[layer], total_in.at[layer, k]))
            for k in ring_far[::-1]:
                far_copy(1, k, total.at[layer], total_in.at[layer, k]).wait_recv()
                value = value + total_in[layer, k]

            own_q, own_k, own_v = [], [], []
            for b in range(seqs):
                mean = value[seqs, 4 + b : 5 + b, :] / model_width
                inverse = lax.rsqrt(mean + EPSILON)
                q = (value[b] * inverse).astype(BF16)
                query[layer, 0, b] = q
                own_q.append(q.astype(F32))
                own_k.append((value[seqs, b : b + 1, :] * inverse).astype(BF16).astype(F32))
                own_v.append((value[seqs, 2 + b : 3 + b, :] * inverse).astype(BF16).astype(F32))
            if layer == 0:
                for k in far_first:
                    slot = opposite(k)
                    start(block_copy(2, k, slot, query.at[layer, 0], query.at[layer, slot]))
            own_score = [
                jnp.sum(own_q[b] * own_k[b], axis=1, keepdims=True) * scale for b in range(seqs)
            ]

            memory_ready()
            if layer == 0:
                attend(layer, [0], mem_near)
                for distance in sorted({hops[k] for k in near_first}):
                    batch = [k for k in near_first if hops[k] == distance]
                    for k in batch:
                        block_copy(2, k, k, query.at[layer, 0], query.at[layer, k]).wait_recv()
                    attend(layer, batch, mem_near)
                    for k in batch:
                        start(block_copy(3, k, k, local.at[layer, k], local_in.at[layer, k]))
                for k in near_first:
                    block_copy(3, k, k, local.at[layer, k], local_in.at[layer, k]).wait_recv()
                outs, stats = combine([local[layer, 0], *[local_in[layer, k] for k in near_first]])
            else:
                outs, stats = attend_block(layer)
            for b in range(seqs):
                merged[layer, b] = outs[b]
            merged[layer, seqs] = stats
            for k in ring_far:
                start(far_copy(4, k, merged.at[layer], merged_in.at[layer, k]))
            for k in ring_far[::-1]:
                far_copy(4, k, merged.at[layer], merged_in.at[layer, k]).wait_recv()
            outs, stats = combine([merged[layer], *[merged_in[layer, k] for k in ring_far]])
            for b in range(seqs):
                peak, summed = stats[:, b : b + 1], stats[:, 2 + b : 3 + b]
                top = jnp.maximum(peak, own_score[b])
                old, own = jnp.exp(peak - top), jnp.exp(own_score[b] - top)
                shared = (outs[b] * old + own * own_v[b]) / (summed * old + own)
                for r in range(group):
                    rows[b : b + 1, r * head : (r + 1) * head] = shared[r : r + 1, :]
            own_rows[layer] = rows[...].astype(BF16)
            for k in far_first:
                slot = opposite(k)
                start(block_copy(5, k, slot, own_rows.at[layer], attended.at[layer, slot]))

            weights_ready()
            branch = jnp.zeros((seqs, done.shape[1] - q_width), F32)
            for k in [0, *near_first]:
                if k:
                    block_copy(5, k, k, own_rows.at[layer], attended.at[layer, k]).wait_recv()
                piece = attended[layer, k] if k else own_rows[layer]
                branch = branch + jnp.dot(
                    piece, weights[q_columns(k), :], preferred_element_type=F32
                )
                if layer == 0:
                    done[:, q_columns(k)] = piece
                else:
                    result[0, :, q_columns(k)] = piece
            return (wide_of() + branch).astype(BF16)

        value = None
        for k in [0, *near_first]:
            copy_to(0, k, k, part.at[k], part_in.at[0, k], block_device(k, 1)).wait_recv()
            value = part_in[0, k] if value is None else value + part_in[0, k]

        def first_hidden():
            cast_hidden.wait_recv()
            return hin[1].astype(F32)

        new = after_projection(
            0, value, first_hidden, cast_mem.wait_recv, w_out_near, cast_out.wait_recv
        )
        done[:, q_width:] = new
        fetch_gain.wait()
        fetch_kv.wait()
        for k in [*far_first, 0]:
            fetch_q(k).wait()
        wide = new.astype(F32)

        def send_one(k):
            if k:
                start(copy_to(6, k, k, part.at[k], part_in.at[1, k], block_device(k, 1)))

        project(wide, lambda k: None, send_one)
        start(cast_done)
        value = part[0]
        for k in near_first:
            copy_to(6, k, k, part.at[k], part_in.at[1, k], block_device(k, 1)).wait_recv()
            value = value + part_in[1, k]

        def memory_ready():
            fetch_mem.wait()
            for k in far_first:
                regroup(k, k).wait_recv()

        new = after_projection(1, value, lambda: wide, memory_ready, w_out, fetch_out.wait)
        result[0, :, q_width:] = new
        for copy in pending:
            copy.wait_send()


def hand_out(heads_total, result, hidden_out, attention_out, held, sem):
    fetch = pltpu.make_async_copy(result, held, sem.at[2])
    attention = pltpu.make_async_copy(held.at[:, :, :heads_total], attention_out, sem.at[0])
    hidden = pltpu.make_async_copy(held.at[:, :, heads_total:], hidden_out, sem.at[1])
    fetch.start()
    fetch.wait()
    attention.start()
    hidden.start()
    attention.wait()
    hidden.wait()


def body(hidden_in, norm_gain, qkv_weight, out_weight, memory, lengths, selected):
    seqs, width = hidden_in.shape
    _, _, heads_kv, blocks_local, _, block, head = memory.shape
    heads_total = out_weight.shape[1]
    group = heads_total // (heads_kv * head)
    x_size, z_size = lax.axis_size(SEQ[0]), lax.axis_size(SEQ[1])
    sizes = (seqs, heads_kv, group, head, block, blocks_local, x_size, z_size)
    members = x_size * PAIR_Z
    far = z_size // PAIR_Z
    tile = (seqs + 1, group, head)
    hbm = pl.BlockSpec(memory_space=pltpu.HBM)
    slots = max(members, far)
    result = pl.pallas_call(
        functools.partial(kernel, sizes),
        out_shape=jax.ShapeDtypeStruct((1, seqs, heads_total + width), BF16),
        in_specs=[hbm] * 7,
        out_specs=pl.BlockSpec(memory_space=pltpu.VMEM),
        scratch_shapes=[
            pltpu.SMEM(lengths.shape, jnp.int32),
            pltpu.VMEM(selected.shape, jnp.int32),
            pltpu.VMEM((1, width), BF16),
            pltpu.VMEM((2, seqs, width), BF16),
            pltpu.VMEM(qkv_weight.shape[1:], BF16),
            pltpu.VMEM(out_weight.shape[1:], BF16),
            pltpu.VMEM(out_weight.shape[1:], BF16),
            pltpu.VMEM((members, seqs, *memory.shape[3:]), BF16),
            pltpu.VMEM((members, seqs, *memory.shape[3:]), BF16),
            pltpu.VMEM(memory.shape[1:], BF16),
            pltpu.VMEM((seqs, heads_kv, group, blocks_local * block), F32),
            pltpu.VMEM((seqs, members, group, blocks_local * block), F32),
            pltpu.VMEM((members, *tile), F32),
            pltpu.VMEM((2, members, *tile), F32),
            pltpu.VMEM((2, *tile), F32),
            pltpu.VMEM((2, far, *tile), F32),
            pltpu.VMEM((2, members, seqs, group, head), BF16),
            pltpu.VMEM((2, members, *tile), F32),
            pltpu.VMEM((2, members, *tile), F32),
            pltpu.VMEM((2, *tile), F32),
            pltpu.VMEM((2, far, *tile), F32),
            pltpu.VMEM((seqs, group * head), F32),
            pltpu.VMEM((2, seqs, group * head), BF16),
            pltpu.VMEM((2, members, seqs, group * head), BF16),
            pltpu.VMEM((seqs, heads_total + width), BF16),
            pltpu.VMEM((seqs, heads_total + width), BF16),
            pltpu.SemaphoreType.DMA((8 + members,)),
            pltpu.SemaphoreType.DMA((2, 4)),
            pltpu.SemaphoreType.REGULAR,
            pltpu.SemaphoreType.DMA((4, members)),
            pltpu.SemaphoreType.DMA((12, slots)),
            pltpu.SemaphoreType.DMA((12, slots)),
        ],
        compiler_params=pltpu.CompilerParams(
            collective_id=0, has_side_effects=True, vmem_limit_bytes=VMEM_BYTES
        ),
        name="decode",
    )(lengths, hidden_in, norm_gain, selected, qkv_weight, out_weight, memory)
    return pl.pallas_call(
        functools.partial(hand_out, heads_total),
        out_shape=(
            jax.ShapeDtypeStruct((1, seqs, width), BF16),
            jax.ShapeDtypeStruct((1, seqs, heads_total), BF16),
        ),
        in_specs=[hbm],
        out_specs=(hbm, hbm),
        scratch_shapes=[pltpu.VMEM(result.shape, BF16), pltpu.SemaphoreType.DMA((3,))],
        name="hand_out",
    )(result)


def solution(mesh):
    z_size = mesh.shape["seq"] // RING_X
    finer = Mesh(
        mesh.devices.reshape(mesh.shape["groups"], RING_X, z_size, mesh.shape["section"]),
        ("groups", *SEQ, "section"),
    )
    in_specs = (
        P("groups", SEQ),
        P("section", SEQ),
        P("section", SEQ, None),
        P("section", None, SEQ),
        P("section", "groups", None, SEQ, None, None, None),
        P("groups"),
        P("groups", None, None),
    )
    out_specs = (P("section", "groups", SEQ), P("section", "groups", None))
    return jax.shard_map(body, mesh=finer, in_specs=in_specs, out_specs=out_specs, check_vma=False)
```

```python
import functools

import jax
import jax.numpy as jnp
from jax import lax
from jax.experimental import pallas as pl
from jax.experimental.pallas import tpu as pltpu
from jax.sharding import Mesh
from jax.sharding import PartitionSpec as P

MESH = pl.DeviceIdType.MESH
EPSILON = 1e-05
FLOOR = -1e30
RING_X = 4
PAIR_Z = 2
SEQ = ("seq_0", "seq_1")
F32, BF16 = jnp.float32, jnp.bfloat16
VMEM_BYTES = 64000000


def kernel(
    sizes,
    lengths_hbm,
    hidden_hbm,
    gain_hbm,
    selected_hbm,
    qkv_hbm,
    out_hbm,
    memory_hbm,
    result,
    lengths,
    selected,
    gain,
    hin,
    w_in,
    w_out,
    w_out_near,
    mem_stage,
    mem_block,
    mem_near,
    live,
    live_block,
    part,
    part_in,
    total,
    total_in,
    query,
    local,
    local_in,
    merged,
    merged_in,
    rows,
    own_rows,
    attended,
    done,
    done_in,
    fetch_sem,
    cast_sem,
    ready_sem,
    group_sem,
    send,
    recv,
):
    seqs, heads_kv, group, head, block, blocks_local, x_size, z_size = sizes
    lanes = group * head
    q_width = heads_kv * lanes
    kv_width = heads_kv * head
    tokens = blocks_local * block
    far_size = z_size // PAIR_Z
    offsets = [(dx, dz) for dx in range(x_size) for dz in range(PAIR_Z)]
    hops = [min(dx, x_size - dx) + dz for dx, dz in offsets]
    near_first = sorted(range(1, len(offsets)), key=lambda k: hops[k])
    far_first = near_first[::-1]
    ring_far = sorted(range(1, far_size), key=lambda k: -min(k, far_size - k))

    x = lax.axis_index(SEQ[0])
    z = lax.axis_index(SEQ[1])
    section = lax.axis_index("section")
    pair = lax.rem(z, PAIR_Z)
    base_z = z - pair
    first_block = (x * z_size + z) * blocks_local
    scale = head ** (-0.5)
    model_width = hin.shape[2] * x_size * z_size

    def in_block(k):
        dx, dz = offsets[k]
        return lax.rem(x + dx, x_size), lax.rem(pair + dz, PAIR_Z)

    def kv_of(k):
        bx, bz = in_block(k)
        return bx * PAIR_Z + bz

    def block_device(k, core):
        bx, bz = in_block(k)
        return {SEQ[0]: bx, SEQ[1]: base_z + bz, "section": core}

    def far_device(k):
        return {SEQ[1]: lax.rem(z + k * PAIR_Z, z_size)}

    def opposite(k):
        dx, dz = offsets[k]
        return offsets.index(((x_size - dx) % x_size, dz))

    barrier = pltpu.get_barrier_semaphore()

    def greet(device):
        pl.semaphore_signal(barrier, inc=1, device_id=device, device_id_type=MESH)

    def copy_to(stage, k, slot, source, target, device):
        return pltpu.make_async_remote_copy(
            src_ref=source,
            dst_ref=target,
            send_sem=send.at[stage, k],
            recv_sem=recv.at[stage, slot],
            device_id=device,
            device_id_type=MESH,
        )

    def cast(number, source, target, core):
        return pltpu.make_async_remote_copy(
            src_ref=source,
            dst_ref=target,
            send_sem=cast_sem.at[0, number],
            recv_sem=cast_sem.at[1, number],
            device_id={"section": core},
            device_id_type=MESH,
        )

    def stage_memory(k):
        return pltpu.make_async_remote_copy(
            src_ref=memory_hbm.at[0, :, kv_of(k)],
            dst_ref=mem_stage.at[k],
            send_sem=group_sem.at[0, k],
            recv_sem=group_sem.at[1, k],
            device_id={"section": 0},
            device_id_type=MESH,
        )

    def regroup(k, slot, piece=()):
        return pltpu.make_async_remote_copy(
            src_ref=mem_stage.at[(k, *piece)],
            dst_ref=mem_block.at[(slot, *piece)],
            send_sem=group_sem.at[2, k],
            recv_sem=group_sem.at[3, slot],
            device_id=block_device(k, 1),
            device_id_type=MESH,
        )

    cast_hidden = cast(0, hidden_hbm, hin.at[1], 1)
    cast_mem = cast(1, memory_hbm.at[0], mem_near, 1)
    cast_out = cast(2, out_hbm.at[0], w_out_near, 1)
    cast_done = cast(3, done, done_in, 0)

    fetch_gain = pltpu.make_async_copy(gain_hbm, gain, fetch_sem.at[0])
    fetch_hidden = pltpu.make_async_copy(hidden_hbm, hin.at[0], fetch_sem.at[1])
    fetch_kv = pltpu.make_async_copy(
        qkv_hbm.at[0, :, pl.ds(q_width, 2 * kv_width)],
        w_in.at[:, pl.ds(q_width, 2 * kv_width)],
        fetch_sem.at[2],
    )

    def q_columns(k):
        return pl.ds(pl.multiple_of(kv_of(k) * lanes, lanes), lanes)

    def fetch_q(k):
        return pltpu.make_async_copy(
            qkv_hbm.at[0, :, q_columns(k)], w_in.at[:, q_columns(k)], fetch_sem.at[8 + k]
        )

    fetch_selected = pltpu.make_async_copy(selected_hbm, selected, fetch_sem.at[3])
    fetch_lengths = pltpu.make_async_copy(lengths_hbm, lengths, fetch_sem.at[4])
    fetch_mem = pltpu.make_async_copy(
        memory_hbm.at[0, :, kv_of(0)], mem_block.at[0], fetch_sem.at[5]
    )
    fetch_out = pltpu.make_async_copy(out_hbm.at[0], w_out, fetch_sem.at[6])

    @pl.when(section == 0)
    def _():
        greet({"section": 1})

    @pl.when(section == 1)
    def _():
        for k in [*far_first, 0]:
            greet(block_device(k, 0))
        for k in ring_far:
            greet(far_device(k))
        for k in far_first:
            greet(block_device(k, 1))

    fetch_gain.start()

    @pl.when(section == 0)
    def _():
        fetch_hidden.start()

    fetch_kv.start()
    for k in [*far_first, 0]:
        fetch_q(k).start()

    def project(wide, ready, send_one):
        normed = (wide * gain[...].astype(F32)).astype(BF16)
        squares = jnp.broadcast_to(jnp.sum(wide * wide, axis=1, keepdims=True), wide.shape)
        order = [*far_first, 0]

        def multiply(k):
            g = kv_of(k)
            at_k = pl.multiple_of(q_width + g * head, head)
            at_v = pl.multiple_of(q_width + kv_width + g * head, head)
            ready(k)
            columns = [q_columns(k), pl.ds(at_k, head), pl.ds(at_v, head)]
            return [jnp.dot(normed, w_in[:, at], preferred_element_type=F32) for at in columns]

        for k in order:
            qs, ks, vs = multiply(k)
            for b in range(seqs):
                for r in range(group):
                    part[k, b, r : r + 1, :] = qs[b : b + 1, r * head : (r + 1) * head]
            part[k, seqs, 0:2, :] = ks
            part[k, seqs, 2:4, :] = vs
            part[k, seqs, 4:6, :] = squares
            part[k, seqs, 6:8, :] = jnp.zeros((2, head), F32)
            send_one(k)

    @pl.when(section == 0)
    def _():
        fetch_gain.wait()
        fetch_hidden.wait()
        fetch_kv.wait()
        sent = []

        def send_one(k):
            if not sent:
                pl.semaphore_wait(barrier, len(offsets))
                pl.semaphore_signal(
                    ready_sem, inc=1, device_id={"section": 1}, device_id_type=MESH
                )
            copy = copy_to(0, k, k, part.at[k], part_in.at[0, k], block_device(k, 1))
            copy.start()
            sent.append(copy)

        project(hin[0].astype(F32), lambda k: fetch_q(k).wait(), send_one)
        cast_hidden.start()
        cast_mem.start()
        cast_out.start()
        for k in far_first:
            stage_memory(k).wait_recv()
            sent.append(regroup(k, opposite(k)))
        piece = block // 4

        def start_piece(ks, n, carry):
            b = n // (blocks_local * 2 * 4)
            j = lax.rem(n // (2 * 4), blocks_local)
            half = lax.rem(n // 4, 2)
            at = pl.ds(pl.multiple_of(lax.rem(n, 4) * piece, piece), piece)
            for k in ks:
                regroup(k, opposite(k), (b, j, half, at)).start()
            return carry

        for dz in (1, 0):
            ks = [k for k in far_first if offsets[k][1] == dz]
            lax.fori_loop(0, seqs * blocks_local * 2 * 4, functools.partial(start_piece, ks), 0)
        for copy in [*sent, cast_hidden, cast_mem, cast_out]:
            copy.wait_send()
        cast_done.wait_recv()
        result[0] = done_in[...]

    @pl.when(section == 1)
    def _():
        pending = []

        def start(copy):
            copy.start()
            pending.append(copy)

        fetch_selected.start()
        fetch_lengths.start()
        fetch_mem.start()
        fetch_out.start()

        fetch_selected.wait()
        fetch_lengths.wait()
        lane = lax.broadcasted_iota(jnp.int32, (heads_kv, tokens), 1)
        for b in range(seqs):
            chosen_ids = selected[b]
            lane_block = first_block + lane // block
            hit = jnp.zeros((heads_kv, tokens), F32)
            for s in range(selected.shape[2]):
                hit = jnp.where(chosen_ids[:, s : s + 1] == lane_block, 1.0, hit)
            hit = jnp.where(first_block * block + lane < lengths[b], hit, 0.0)
            for g in range(heads_kv):
                live[b, g] = jnp.broadcast_to(hit[g : g + 1, :], (group, tokens))

        pl.semaphore_wait(ready_sem, 1)
        for k in far_first:
            start(stage_memory(k))

        row = lax.broadcasted_iota(jnp.int32, (len(offsets), tokens), 0)
        row_lane = lax.broadcasted_iota(jnp.int32, (len(offsets), tokens), 1)
        row_first = jnp.zeros((len(offsets), tokens), jnp.int32)
        for k in range(len(offsets)):
            bx, bz = in_block(k)
            row_first = jnp.where(
                row == k, (bx * z_size + base_z + bz) * blocks_local, row_first
            )
        for b in range(seqs):
            chosen_ids = selected[b, pl.ds(kv_of(0), 1), :]
            hit = jnp.zeros((len(offsets), tokens), F32)
            for s in range(selected.shape[2]):
                hit = jnp.where(
                    chosen_ids[:, s : s + 1] == row_first + row_lane // block, 1.0, hit
                )
            hit = jnp.where(row_first * block + row_lane < lengths[b], hit, 0.0)
            for k in range(len(offsets)):
                live_block[b, k] = jnp.broadcast_to(hit[k : k + 1, :], (group, tokens))
        stat_lane = lax.broadcasted_iota(jnp.int32, (group, head), 1)
        def score_of(q, keys, mask):
            score = lax.dot_general(
                q, keys, (((1,), (1,)), ((), ())), preferred_element_type=F32
            )
            return jnp.where(mask, score * scale, FLOOR)

        def mix(weight, values):
            high = weight.astype(BF16)
            low = (weight - high.astype(F32)).astype(BF16)
            mixed = jnp.dot(
                jnp.concatenate([high, low], axis=0), values, preferred_element_type=F32
            )
            return mixed[:group] + mixed[group:]

        def stats_of(peaks, sums):
            stats = jnp.where(stat_lane < 3, sums[0], sums[1])
            stats = jnp.where(stat_lane < 2, peaks[1], stats)
            return jnp.where(stat_lane < 1, peaks[0], stats)

        def attend(layer, ks, memory):
            pairs = [(k, b) for k in ks for b in range(seqs)]
            heads = [kv_of(k) for k, b in pairs]
            masks = [live[b, g] > 0.5 for (k, b), g in zip(pairs, heads)]
            scores = [
                score_of(query[layer, k, b], memory[b, g, :, 0].reshape(tokens, head), mask)
                for (k, b), g, mask in zip(pairs, heads, masks)
            ]
            peaks = [jnp.max(score, axis=1, keepdims=True) for score in scores]
            weights = [
                jnp.where(mask, jnp.exp(score - peak), 0.0)
                for score, peak, mask in zip(scores, peaks, masks)
            ]
            sums = [jnp.sum(weight, axis=1, keepdims=True) for weight in weights]
            for (k, b), g, weight in zip(pairs, heads, weights):
                local[layer, k, b] = mix(weight, memory[b, g, :, 1].reshape(tokens, head))
            for n, k in enumerate(ks):
                at = slice(n * seqs, (n + 1) * seqs)
                local[layer, k, seqs] = stats_of(peaks[at], sums[at])

        def attend_block(layer):
            members = range(len(offsets))
            outs, peaks, sums = [], [], []
            for b in range(seqs):
                masks = [live_block[b, k] > 0.5 for k in members]
                scores = [
                    score_of(
                        query[layer, 0, b], mem_block[k, b, :, 0].reshape(tokens, head), masks[k]
                    )
                    for k in members
                ]
                highest = scores[0]
                for score in scores[1:]:
                    highest = jnp.maximum(highest, score)
                peak = jnp.max(highest, axis=1, keepdims=True)
                out = jnp.zeros((group, head), F32)
                total_weight = jnp.zeros((group, tokens), F32)
                for k in members:
                    weight = jnp.where(masks[k], jnp.exp(scores[k] - peak), 0.0)
                    total_weight = total_weight + weight
                    out = out + mix(weight, mem_block[k, b, :, 1].reshape(tokens, head))
                outs.append(out)
                peaks.append(peak)
                sums.append(jnp.sum(total_weight, axis=1, keepdims=True))
            return outs, stats_of(peaks, sums)

        def combine(parts):
            top = parts[0][seqs]
            for p in parts[1:]:
                top = jnp.maximum(top, p[seqs])
            sums = jnp.zeros((group, head), F32)
            outs = [jnp.zeros((group, head), F32) for _ in range(seqs)]
            for p in parts:
                factor = jnp.where(stat_lane < 2, jnp.exp(jnp.minimum(p[seqs] - top, 0.0)), 0.0)
                wides = [
                    jnp.broadcast_to(factor[:, b : b + 1], (group, head)) for b in range(seqs)
                ]
                sums = sums + p[seqs] * jnp.where(stat_lane < 3, wides[0], wides[1])
                outs = [outs[b] + p[b] * wides[b] for b in range(seqs)]
            return outs, jnp.where(stat_lane < 2, top, sums)

        def after_projection(layer, value, wide_of, memory_ready, weights, weights_ready):
            stage = 6 * layer
            total[layer] = value
            if layer == 0:
                pl.semaphore_wait(barrier, len(ring_far) + len(far_first) + 1)

            def far_copy(n, k, source, target):
                return copy_to(stage + n, k, k, source, target, far_device(k))

            def block_copy(n, k, slot, source, target):
                return copy_to(stage + n, k, slot, source, target, block_device(k, 1))

            for k in ring_far:
                start(far_copy(1, k, total.at[layer], total_in.at[layer, k]))
            for k in ring_far[::-1]:
                far_copy(1, k, total.at[layer], total_in.at[layer, k]).wait_recv()
                value = value + total_in[layer, k]

            own_q, own_k, own_v = [], [], []
            for b in range(seqs):
                mean = value[seqs, 4 + b : 5 + b, :] / model_width
                inverse = lax.rsqrt(mean + EPSILON)
                q = (value[b] * inverse).astype(BF16)
                query[layer, 0, b] = q
                own_q.append(q.astype(F32))
                own_k.append((value[seqs, b : b + 1, :] * inverse).astype(BF16).astype(F32))
                own_v.append((value[seqs, 2 + b : 3 + b, :] * inverse).astype(BF16).astype(F32))
            if layer == 0:
                for k in far_first:
                    slot = opposite(k)
                    start(block_copy(2, k, slot, query.at[layer, 0], query.at[layer, slot]))
            own_score = [
                jnp.sum(own_q[b] * own_k[b], axis=1, keepdims=True) * scale for b in range(seqs)
            ]

            memory_ready()
            if layer == 0:
                attend(layer, [0], mem_near)
                for distance in sorted({hops[k] for k in near_first}):
                    batch = [k for k in near_first if hops[k] == distance]
                    for k in batch:
                        block_copy(2, k, k, query.at[layer, 0], query.at[layer, k]).wait_recv()
                    attend(layer, batch, mem_near)
                    for k in batch:
                        start(block_copy(3, k, k, local.at[layer, k], local_in.at[layer, k]))
                for k in near_first:
                    block_copy(3, k, k, local.at[layer, k], local_in.at[layer, k]).wait_recv()
                outs, stats = combine([local[layer, 0], *[local_in[layer, k] for k in near_first]])
            else:
                outs, stats = attend_block(layer)
            for b in range(seqs):
                merged[layer, b] = outs[b]
            merged[layer, seqs] = stats
            for k in ring_far:
                start(far_copy(4, k, merged.at[layer], merged_in.at[layer, k]))
            for k in ring_far[::-1]:
                far_copy(4, k, merged.at[layer], merged_in.at[layer, k]).wait_recv()
            outs, stats = combine([merged[layer], *[merged_in[layer, k] for k in ring_far]])
            for b in range(seqs):
                peak, summed = stats[:, b : b + 1], stats[:, 2 + b : 3 + b]
                top = jnp.maximum(peak, own_score[b])
                old, own = jnp.exp(peak - top), jnp.exp(own_score[b] - top)
                shared = (outs[b] * old + own * own_v[b]) / (summed * old + own)
                for r in range(group):
                    rows[b : b + 1, r * head : (r + 1) * head] = shared[r : r + 1, :]
            own_rows[layer] = rows[...].astype(BF16)
            for k in far_first:
                slot = opposite(k)
                start(block_copy(5, k, slot, own_rows.at[layer], attended.at[layer, slot]))

            weights_ready()
            branch = jnp.zeros((seqs, done.shape[1] - q_width), F32)
            for k in [0, *near_first]:
                if k:
                    block_copy(5, k, k, own_rows.at[layer], attended.at[layer, k]).wait_recv()
                piece = attended[layer, k] if k else own_rows[layer]
                branch = branch + jnp.dot(
                    piece, weights[q_columns(k), :], preferred_element_type=F32
                )
                if layer == 0:
                    done[:, q_columns(k)] = piece
                else:
                    result[0, :, q_columns(k)] = piece
            return (wide_of() + branch).astype(BF16)

        value = None
        for k in [0, *near_first]:
            copy_to(0, k, k, part.at[k], part_in.at[0, k], block_device(k, 1)).wait_recv()
            value = part_in[0, k] if value is None else value + part_in[0, k]

        def first_hidden():
            cast_hidden.wait_recv()
            return hin[1].astype(F32)

        new = after_projection(
            0, value, first_hidden, cast_mem.wait_recv, w_out_near, cast_out.wait_recv
        )
        done[:, q_width:] = new
        fetch_gain.wait()
        fetch_kv.wait()
        for k in [*far_first, 0]:
            fetch_q(k).wait()
        wide = new.astype(F32)

        def send_one(k):
            if k:
                start(copy_to(6, k, k, part.at[k], part_in.at[1, k], block_device(k, 1)))

        project(wide, lambda k: None, send_one)
        start(cast_done)
        value = part[0]
        for k in near_first:
            copy_to(6, k, k, part.at[k], part_in.at[1, k], block_device(k, 1)).wait_recv()
            value = value + part_in[1, k]

        def memory_ready():
            fetch_mem.wait()
            for k in far_first:
                regroup(k, k).wait_recv()

        new = after_projection(1, value, lambda: wide, memory_ready, w_out, fetch_out.wait)
        result[0, :, q_width:] = new
        for copy in pending:
            copy.wait_send()


def hand_out(heads_total, result, hidden_out, attention_out, held, sem):
    fetch = pltpu.make_async_copy(result, held, sem.at[2])
    attention = pltpu.make_async_copy(held.at[:, :, :heads_total], attention_out, sem.at[0])
    hidden = pltpu.make_async_copy(held.at[:, :, heads_total:], hidden_out, sem.at[1])
    fetch.start()
    fetch.wait()
    attention.start()
    hidden.start()
    attention.wait()
    hidden.wait()


def body(hidden_in, norm_gain, qkv_weight, out_weight, memory, lengths, selected):
    seqs, width = hidden_in.shape
    _, _, heads_kv, blocks_local, _, block, head = memory.shape
    heads_total = out_weight.shape[1]
    group = heads_total // (heads_kv * head)
    x_size, z_size = lax.axis_size(SEQ[0]), lax.axis_size(SEQ[1])
    sizes = (seqs, heads_kv, group, head, block, blocks_local, x_size, z_size)
    members = x_size * PAIR_Z
    far = z_size // PAIR_Z
    tile = (seqs + 1, group, head)
    hbm = pl.BlockSpec(memory_space=pltpu.HBM)
    slots = max(members, far)
    result = pl.pallas_call(
        functools.partial(kernel, sizes),
        out_shape=jax.ShapeDtypeStruct((1, seqs, heads_total + width), BF16),
        in_specs=[hbm] * 7,
        out_specs=pl.BlockSpec(memory_space=pltpu.VMEM),
        scratch_shapes=[
            pltpu.SMEM(lengths.shape, jnp.int32),
            pltpu.VMEM(selected.shape, jnp.int32),
            pltpu.VMEM((1, width), BF16),
            pltpu.VMEM((2, seqs, width), BF16),
            pltpu.VMEM(qkv_weight.shape[1:], BF16),
            pltpu.VMEM(out_weight.shape[1:], BF16),
            pltpu.VMEM(out_weight.shape[1:], BF16),
            pltpu.VMEM((members, seqs, *memory.shape[3:]), BF16),
            pltpu.VMEM((members, seqs, *memory.shape[3:]), BF16),
            pltpu.VMEM(memory.shape[1:], BF16),
            pltpu.VMEM((seqs, heads_kv, group, blocks_local * block), F32),
            pltpu.VMEM((seqs, members, group, blocks_local * block), F32),
            pltpu.VMEM((members, *tile), F32),
            pltpu.VMEM((2, members, *tile), F32),
            pltpu.VMEM((2, *tile), F32),
            pltpu.VMEM((2, far, *tile), F32),
            pltpu.VMEM((2, members, seqs, group, head), BF16),
            pltpu.VMEM((2, members, *tile), F32),
            pltpu.VMEM((2, members, *tile), F32),
            pltpu.VMEM((2, *tile), F32),
            pltpu.VMEM((2, far, *tile), F32),
            pltpu.VMEM((seqs, group * head), F32),
            pltpu.VMEM((2, seqs, group * head), BF16),
            pltpu.VMEM((2, members, seqs, group * head), BF16),
            pltpu.VMEM((seqs, heads_total + width), BF16),
            pltpu.VMEM((seqs, heads_total + width), BF16),
            pltpu.SemaphoreType.DMA((8 + members,)),
            pltpu.SemaphoreType.DMA((2, 4)),
            pltpu.SemaphoreType.REGULAR,
            pltpu.SemaphoreType.DMA((4, members)),
            pltpu.SemaphoreType.DMA((12, slots)),
            pltpu.SemaphoreType.DMA((12, slots)),
        ],
        compiler_params=pltpu.CompilerParams(
            collective_id=0, has_side_effects=True, vmem_limit_bytes=VMEM_BYTES
        ),
        name="decode",
    )(lengths, hidden_in, norm_gain, selected, qkv_weight, out_weight, memory)
    return pl.pallas_call(
        functools.partial(hand_out, heads_total),
        out_shape=(
            jax.ShapeDtypeStruct((1, seqs, width), BF16),
            jax.ShapeDtypeStruct((1, seqs, heads_total), BF16),
        ),
        in_specs=[hbm],
        out_specs=(hbm, hbm),
        scratch_shapes=[pltpu.VMEM(result.shape, BF16), pltpu.SemaphoreType.DMA((3,))],
        name="hand_out",
    )(result)


def solution(mesh):
    z_size = mesh.shape["seq"] // RING_X
    finer = Mesh(
        mesh.devices.reshape(mesh.shape["groups"], RING_X, z_size, mesh.shape["section"]),
        ("groups", *SEQ, "section"),
    )
    in_specs = (
        P("groups", SEQ),
        P("section", SEQ),
        P("section", SEQ, None),
        P("section", None, SEQ),
        P("section", "groups", None, SEQ, None, None, None),
        P("groups"),
        P("groups", None, None),
    )
    out_specs = (P("section", "groups", SEQ), P("section", "groups", None))
    return jax.shard_map(body, mesh=finer, in_specs=in_specs, out_specs=out_specs, check_vma=False)
```

```python
import functools

import jax
import jax.numpy as jnp
from jax import lax
from jax.experimental import pallas as pl
from jax.experimental.pallas import tpu as pltpu
from jax.sharding import Mesh
from jax.sharding import PartitionSpec as P

MESH = pl.DeviceIdType.MESH
EPSILON = 1e-05
FLOOR = -1e30
RING_X = 4
PAIR_Z = 2
SEQ = ("seq_0", "seq_1")
F32, BF16 = jnp.float32, jnp.bfloat16
VMEM_BYTES = 64000000


def kernel(
    sizes,
    lengths_hbm,
    hidden_hbm,
    gain_hbm,
    selected_hbm,
    qkv_hbm,
    out_hbm,
    memory_hbm,
    result,
    lengths,
    selected,
    gain,
    hin,
    w_in,
    w_out,
    w_out_near,
    mem_stage,
    mem_block,
    mem_near,
    live,
    live_block,
    part,
    part_in,
    total,
    total_in,
    query,
    local,
    local_in,
    merged,
    merged_in,
    rows,
    own_rows,
    attended,
    done,
    done_in,
    fetch_sem,
    cast_sem,
    ready_sem,
    group_sem,
    send,
    recv,
):
    seqs, heads_kv, group, head, block, blocks_local, x_size, z_size = sizes
    lanes = group * head
    q_width = heads_kv * lanes
    kv_width = heads_kv * head
    tokens = blocks_local * block
    far_size = z_size // PAIR_Z
    offsets = [(dx, dz) for dx in range(x_size) for dz in range(PAIR_Z)]
    hops = [min(dx, x_size - dx) + dz for dx, dz in offsets]
    near_first = sorted(range(1, len(offsets)), key=lambda k: hops[k])
    far_first = near_first[::-1]
    ring_far = sorted(range(1, far_size), key=lambda k: -min(k, far_size - k))

    x = lax.axis_index(SEQ[0])
    z = lax.axis_index(SEQ[1])
    section = lax.axis_index("section")
    pair = lax.rem(z, PAIR_Z)
    base_z = z - pair
    first_block = (x * z_size + z) * blocks_local
    scale = head ** (-0.5)
    model_width = hin.shape[2] * x_size * z_size

    def in_block(k):
        dx, dz = offsets[k]
        return lax.rem(x + dx, x_size), lax.rem(pair + dz, PAIR_Z)

    def kv_of(k):
        bx, bz = in_block(k)
        return bx * PAIR_Z + bz

    def block_device(k, core):
        bx, bz = in_block(k)
        return {SEQ[0]: bx, SEQ[1]: base_z + bz, "section": core}

    def far_device(k):
        return {SEQ[1]: lax.rem(z + k * PAIR_Z, z_size)}

    def opposite(k):
        dx, dz = offsets[k]
        return offsets.index(((x_size - dx) % x_size, dz))

    barrier = pltpu.get_barrier_semaphore()

    def greet(device):
        pl.semaphore_signal(barrier, inc=1, device_id=device, device_id_type=MESH)

    def copy_to(stage, k, slot, source, target, device):
        return pltpu.make_async_remote_copy(
            src_ref=source,
            dst_ref=target,
            send_sem=send.at[stage, k],
            recv_sem=recv.at[stage, slot],
            device_id=device,
            device_id_type=MESH,
        )

    def cast(number, source, target, core):
        return pltpu.make_async_remote_copy(
            src_ref=source,
            dst_ref=target,
            send_sem=cast_sem.at[0, number],
            recv_sem=cast_sem.at[1, number],
            device_id={"section": core},
            device_id_type=MESH,
        )

    def stage_memory(k):
        return pltpu.make_async_remote_copy(
            src_ref=memory_hbm.at[0, :, kv_of(k)],
            dst_ref=mem_stage.at[k],
            send_sem=group_sem.at[0, k],
            recv_sem=group_sem.at[1, k],
            device_id={"section": 0},
            device_id_type=MESH,
        )

    def regroup(k, slot, piece=()):
        return pltpu.make_async_remote_copy(
            src_ref=mem_stage.at[(k, *piece)],
            dst_ref=mem_block.at[(slot, *piece)],
            send_sem=group_sem.at[2, k],
            recv_sem=group_sem.at[3, slot],
            device_id=block_device(k, 1),
            device_id_type=MESH,
        )

    cast_hidden = cast(0, hidden_hbm, hin.at[1], 1)
    cast_mem = cast(1, memory_hbm.at[0], mem_near, 1)
    cast_out = cast(2, out_hbm.at[0], w_out_near, 1)
    cast_done = cast(3, done, done_in, 0)

    fetch_gain = pltpu.make_async_copy(gain_hbm, gain, fetch_sem.at[0])
    fetch_hidden = pltpu.make_async_copy(hidden_hbm, hin.at[0], fetch_sem.at[1])
    fetch_kv = pltpu.make_async_copy(
        qkv_hbm.at[0, :, pl.ds(q_width, 2 * kv_width)],
        w_in.at[:, pl.ds(q_width, 2 * kv_width)],
        fetch_sem.at[2],
    )

    def q_columns(k):
        return pl.ds(pl.multiple_of(kv_of(k) * lanes, lanes), lanes)

    def fetch_q(k):
        return pltpu.make_async_copy(
            qkv_hbm.at[0, :, q_columns(k)], w_in.at[:, q_columns(k)], fetch_sem.at[8 + k]
        )

    fetch_selected = pltpu.make_async_copy(selected_hbm, selected, fetch_sem.at[3])
    fetch_lengths = pltpu.make_async_copy(lengths_hbm, lengths, fetch_sem.at[4])
    fetch_mem = pltpu.make_async_copy(
        memory_hbm.at[0, :, kv_of(0)], mem_block.at[0], fetch_sem.at[5]
    )
    fetch_out = pltpu.make_async_copy(out_hbm.at[0], w_out, fetch_sem.at[6])

    @pl.when(section == 0)
    def _():
        greet({"section": 1})

    @pl.when(section == 1)
    def _():
        for k in [*far_first, 0]:
            greet(block_device(k, 0))
        for k in ring_far:
            greet(far_device(k))
        for k in far_first:
            greet(block_device(k, 1))

    fetch_gain.start()

    @pl.when(section == 0)
    def _():
        fetch_hidden.start()

    fetch_kv.start()
    for k in [*far_first, 0]:
        fetch_q(k).start()

    def project(wide, ready, send_one):
        normed = (wide * gain[...].astype(F32)).astype(BF16)
        squares = jnp.broadcast_to(jnp.sum(wide * wide, axis=1, keepdims=True), wide.shape)
        order = [*far_first, 0]

        def multiply(k):
            g = kv_of(k)
            at_k = pl.multiple_of(q_width + g * head, head)
            at_v = pl.multiple_of(q_width + kv_width + g * head, head)
            ready(k)
            columns = [q_columns(k), pl.ds(at_k, head), pl.ds(at_v, head)]
            return [jnp.dot(normed, w_in[:, at], preferred_element_type=F32) for at in columns]

        for k in order:
            qs, ks, vs = multiply(k)
            for b in range(seqs):
                for r in range(group):
                    part[k, b, r : r + 1, :] = qs[b : b + 1, r * head : (r + 1) * head]
            part[k, seqs, 0:2, :] = ks
            part[k, seqs, 2:4, :] = vs
            part[k, seqs, 4:6, :] = squares
            part[k, seqs, 6:8, :] = jnp.zeros((2, head), F32)
            send_one(k)

    @pl.when(section == 0)
    def _():
        fetch_gain.wait()
        fetch_hidden.wait()
        fetch_kv.wait()
        sent = []

        def send_one(k):
            if not sent:
                pl.semaphore_wait(barrier, len(offsets))
                pl.semaphore_signal(
                    ready_sem, inc=1, device_id={"section": 1}, device_id_type=MESH
                )
            copy = copy_to(0, k, k, part.at[k], part_in.at[0, k], block_device(k, 1))
            copy.start()
            sent.append(copy)

        project(hin[0].astype(F32), lambda k: fetch_q(k).wait(), send_one)
        cast_hidden.start()
        cast_mem.start()
        cast_out.start()
        for k in far_first:
            stage_memory(k).wait_recv()
            sent.append(regroup(k, opposite(k)))
        piece = block // 4

        def start_piece(ks, n, carry):
            b = n // (blocks_local * 2 * 4)
            j = lax.rem(n // (2 * 4), blocks_local)
            half = lax.rem(n // 4, 2)
            at = pl.ds(pl.multiple_of(lax.rem(n, 4) * piece, piece), piece)
            for k in ks:
                regroup(k, opposite(k), (b, j, half, at)).start()
            return carry

        for dz in (1, 0):
            ks = [k for k in far_first if offsets[k][1] == dz]
            lax.fori_loop(0, seqs * blocks_local * 2 * 4, functools.partial(start_piece, ks), 0)
        for copy in [*sent, cast_hidden, cast_mem, cast_out]:
            copy.wait_send()
        cast_done.wait_recv()
        result[0] = done_in[...]

    @pl.when(section == 1)
    def _():
        pending = []

        def start(copy):
            copy.start()
            pending.append(copy)

        fetch_selected.start()
        fetch_lengths.start()
        fetch_mem.start()
        fetch_out.start()

        fetch_selected.wait()
        fetch_lengths.wait()
        lane = lax.broadcasted_iota(jnp.int32, (heads_kv, tokens), 1)
        for b in range(seqs):
            chosen_ids = selected[b]
            lane_block = first_block + lane // block
            hit = jnp.zeros((heads_kv, tokens), F32)
            for s in range(selected.shape[2]):
                hit = jnp.where(chosen_ids[:, s : s + 1] == lane_block, 1.0, hit)
            hit = jnp.where(first_block * block + lane < lengths[b], hit, 0.0)
            for g in range(heads_kv):
                live[b, g] = jnp.broadcast_to(hit[g : g + 1, :], (group, tokens))

        pl.semaphore_wait(ready_sem, 1)
        for k in far_first:
            start(stage_memory(k))

        row = lax.broadcasted_iota(jnp.int32, (len(offsets), tokens), 0)
        row_lane = lax.broadcasted_iota(jnp.int32, (len(offsets), tokens), 1)
        row_first = jnp.zeros((len(offsets), tokens), jnp.int32)
        for k in range(len(offsets)):
            bx, bz = in_block(k)
            row_first = jnp.where(
                row == k, (bx * z_size + base_z + bz) * blocks_local, row_first
            )
        for b in range(seqs):
            chosen_ids = selected[b, pl.ds(kv_of(0), 1), :]
            hit = jnp.zeros((len(offsets), tokens), F32)
            for s in range(selected.shape[2]):
                hit = jnp.where(
                    chosen_ids[:, s : s + 1] == row_first + row_lane // block, 1.0, hit
                )
            hit = jnp.where(row_first * block + row_lane < lengths[b], hit, 0.0)
            for k in range(len(offsets)):
                live_block[b, k] = jnp.broadcast_to(hit[k : k + 1, :], (group, tokens))
        stat_lane = lax.broadcasted_iota(jnp.int32, (group, head), 1)
        def score_of(q, keys, mask):
            score = lax.dot_general(
                q, keys, (((1,), (1,)), ((), ())), preferred_element_type=F32
            )
            return jnp.where(mask, score * scale, FLOOR)

        def mix(weight, values):
            high = weight.astype(BF16)
            low = (weight - high.astype(F32)).astype(BF16)
            mixed = jnp.dot(
                jnp.concatenate([high, low], axis=0), values, preferred_element_type=F32
            )
            return mixed[:group] + mixed[group:]

        def stats_of(peaks, sums):
            stats = jnp.where(stat_lane < 3, sums[0], sums[1])
            stats = jnp.where(stat_lane < 2, peaks[1], stats)
            return jnp.where(stat_lane < 1, peaks[0], stats)

        def attend(layer, ks, memory):
            pairs = [(k, b) for k in ks for b in range(seqs)]
            heads = [kv_of(k) for k, b in pairs]
            masks = [live[b, g] > 0.5 for (k, b), g in zip(pairs, heads)]
            scores = [
                score_of(query[layer, k, b], memory[b, g, :, 0].reshape(tokens, head), mask)
                for (k, b), g, mask in zip(pairs, heads, masks)
            ]
            peaks = [jnp.max(score, axis=1, keepdims=True) for score in scores]
            weights = [
                jnp.where(mask, jnp.exp(score - peak), 0.0)
                for score, peak, mask in zip(scores, peaks, masks)
            ]
            sums = [jnp.sum(weight, axis=1, keepdims=True) for weight in weights]
            for (k, b), g, weight in zip(pairs, heads, weights):
                local[layer, k, b] = mix(weight, memory[b, g, :, 1].reshape(tokens, head))
            for n, k in enumerate(ks):
                at = slice(n * seqs, (n + 1) * seqs)
                local[layer, k, seqs] = stats_of(peaks[at], sums[at])

        def attend_block(layer):
            members = range(len(offsets))
            outs, peaks, sums = [], [], []
            for b in range(seqs):
                masks = [live_block[b, k] > 0.5 for k in members]
                scores = [
                    score_of(
                        query[layer, 0, b], mem_block[k, b, :, 0].reshape(tokens, head), masks[k]
                    )
                    for k in members
                ]
                highest = scores[0]
                for score in scores[1:]:
                    highest = jnp.maximum(highest, score)
                peak = jnp.max(highest, axis=1, keepdims=True)
                out = jnp.zeros((group, head), F32)
                total_weight = jnp.zeros((group, tokens), F32)
                for k in members:
                    weight = jnp.where(masks[k], jnp.exp(scores[k] - peak), 0.0)
                    total_weight = total_weight + weight
                    out = out + mix(weight, mem_block[k, b, :, 1].reshape(tokens, head))
                outs.append(out)
                peaks.append(peak)
                sums.append(jnp.sum(total_weight, axis=1, keepdims=True))
            return outs, stats_of(peaks, sums)

        def combine(parts):
            top = parts[0][seqs]
            for p in parts[1:]:
                top = jnp.maximum(top, p[seqs])
            sums = jnp.zeros((group, head), F32)
            outs = [jnp.zeros((group, head), F32) for _ in range(seqs)]
            for p in parts:
                factor = jnp.where(stat_lane < 2, jnp.exp(jnp.minimum(p[seqs] - top, 0.0)), 0.0)
                wides = [
                    jnp.broadcast_to(factor[:, b : b + 1], (group, head)) for b in range(seqs)
                ]
                sums = sums + p[seqs] * jnp.where(stat_lane < 3, wides[0], wides[1])
                outs = [outs[b] + p[b] * wides[b] for b in range(seqs)]
            return outs, jnp.where(stat_lane < 2, top, sums)

        def after_projection(layer, value, wide_of, memory_ready, weights, weights_ready):
            stage = 6 * layer
            total[layer] = value
            if layer == 0:
                pl.semaphore_wait(barrier, len(ring_far) + len(far_first) + 1)

            def far_copy(n, k, source, target):
                return copy_to(stage + n, k, k, source, target, far_device(k))

            def block_copy(n, k, slot, source, target):
                return copy_to(stage + n, k, slot, source, target, block_device(k, 1))

            for k in ring_far:
                start(far_copy(1, k, total.at[layer], total_in.at[layer, k]))
            for k in ring_far[::-1]:
                far_copy(1, k, total.at[layer], total_in.at[layer, k]).wait_recv()
                value = value + total_in[layer, k]

            own_q, own_k, own_v = [], [], []
            for b in range(seqs):
                mean = value[seqs, 4 + b : 5 + b, :] / model_width
                inverse = lax.rsqrt(mean + EPSILON)
                q = (value[b] * inverse).astype(BF16)
                query[layer, 0, b] = q
                own_q.append(q.astype(F32))
                own_k.append((value[seqs, b : b + 1, :] * inverse).astype(BF16).astype(F32))
                own_v.append((value[seqs, 2 + b : 3 + b, :] * inverse).astype(BF16).astype(F32))
            if layer == 0:
                for k in far_first:
                    slot = opposite(k)
                    start(block_copy(2, k, slot, query.at[layer, 0], query.at[layer, slot]))
            own_score = [
                jnp.sum(own_q[b] * own_k[b], axis=1, keepdims=True) * scale for b in range(seqs)
            ]

            memory_ready()
            if layer == 0:
                attend(layer, [0], mem_near)
                for close in (True, False):
                    batch = [k for k in near_first if (hops[k] == 1) == close]
                    for k in batch:
                        block_copy(2, k, k, query.at[layer, 0], query.at[layer, k]).wait_recv()
                    attend(layer, batch, mem_near)
                    for k in batch:
                        start(block_copy(3, k, k, local.at[layer, k], local_in.at[layer, k]))
                for k in near_first:
                    block_copy(3, k, k, local.at[layer, k], local_in.at[layer, k]).wait_recv()
                outs, stats = combine([local[layer, 0], *[local_in[layer, k] for k in near_first]])
            else:
                outs, stats = attend_block(layer)
            for b in range(seqs):
                merged[layer, b] = outs[b]
            merged[layer, seqs] = stats
            for k in ring_far:
                start(far_copy(4, k, merged.at[layer], merged_in.at[layer, k]))
            for k in ring_far[::-1]:
                far_copy(4, k, merged.at[layer], merged_in.at[layer, k]).wait_recv()
            outs, stats = combine([merged[layer], *[merged_in[layer, k] for k in ring_far]])
            for b in range(seqs):
                peak, summed = stats[:, b : b + 1], stats[:, 2 + b : 3 + b]
                top = jnp.maximum(peak, own_score[b])
                old, own = jnp.exp(peak - top), jnp.exp(own_score[b] - top)
                shared = (outs[b] * old + own * own_v[b]) / (summed * old + own)
                for r in range(group):
                    rows[b : b + 1, r * head : (r + 1) * head] = shared[r : r + 1, :]
            own_rows[layer] = rows[...].astype(BF16)
            for k in far_first:
                slot = opposite(k)
                start(block_copy(5, k, slot, own_rows.at[layer], attended.at[layer, slot]))

            weights_ready()
            branch = jnp.zeros((seqs, done.shape[1] - q_width), F32)
            for k in [0, *near_first]:
                if k:
                    block_copy(5, k, k, own_rows.at[layer], attended.at[layer, k]).wait_recv()
                piece = attended[layer, k] if k else own_rows[layer]
                branch = branch + jnp.dot(
                    piece, weights[q_columns(k), :], preferred_element_type=F32
                )
                if layer == 0:
                    done[:, q_columns(k)] = piece
                else:
                    result[0, :, q_columns(k)] = piece
            return (wide_of() + branch).astype(BF16)

        value = None
        for k in [0, *near_first]:
            copy_to(0, k, k, part.at[k], part_in.at[0, k], block_device(k, 1)).wait_recv()
            value = part_in[0, k] if value is None else value + part_in[0, k]

        def first_hidden():
            cast_hidden.wait_recv()
            return hin[1].astype(F32)

        new = after_projection(
            0, value, first_hidden, cast_mem.wait_recv, w_out_near, cast_out.wait_recv
        )
        done[:, q_width:] = new
        fetch_gain.wait()
        fetch_kv.wait()
        for k in [*far_first, 0]:
            fetch_q(k).wait()
        wide = new.astype(F32)

        def send_one(k):
            if k:
                start(copy_to(6, k, k, part.at[k], part_in.at[1, k], block_device(k, 1)))

        project(wide, lambda k: None, send_one)
        start(cast_done)
        value = part[0]
        for k in near_first:
            copy_to(6, k, k, part.at[k], part_in.at[1, k], block_device(k, 1)).wait_recv()
            value = value + part_in[1, k]

        def memory_ready():
            fetch_mem.wait()
            for k in far_first:
                regroup(k, k).wait_recv()

        new = after_projection(1, value, lambda: wide, memory_ready, w_out, fetch_out.wait)
        result[0, :, q_width:] = new
        for copy in pending:
            copy.wait_send()


def hand_out(heads_total, result, hidden_out, attention_out, held, sem):
    fetch = pltpu.make_async_copy(result, held, sem.at[2])
    attention = pltpu.make_async_copy(held.at[:, :, :heads_total], attention_out, sem.at[0])
    hidden = pltpu.make_async_copy(held.at[:, :, heads_total:], hidden_out, sem.at[1])
    fetch.start()
    fetch.wait()
    attention.start()
    hidden.start()
    attention.wait()
    hidden.wait()


def body(hidden_in, norm_gain, qkv_weight, out_weight, memory, lengths, selected):
    seqs, width = hidden_in.shape
    _, _, heads_kv, blocks_local, _, block, head = memory.shape
    heads_total = out_weight.shape[1]
    group = heads_total // (heads_kv * head)
    x_size, z_size = lax.axis_size(SEQ[0]), lax.axis_size(SEQ[1])
    sizes = (seqs, heads_kv, group, head, block, blocks_local, x_size, z_size)
    members = x_size * PAIR_Z
    far = z_size // PAIR_Z
    tile = (seqs + 1, group, head)
    hbm = pl.BlockSpec(memory_space=pltpu.HBM)
    slots = max(members, far)
    result = pl.pallas_call(
        functools.partial(kernel, sizes),
        out_shape=jax.ShapeDtypeStruct((1, seqs, heads_total + width), BF16),
        in_specs=[hbm] * 7,
        out_specs=pl.BlockSpec(memory_space=pltpu.VMEM),
        scratch_shapes=[
            pltpu.SMEM(lengths.shape, jnp.int32),
            pltpu.VMEM(selected.shape, jnp.int32),
            pltpu.VMEM((1, width), BF16),
            pltpu.VMEM((2, seqs, width), BF16),
            pltpu.VMEM(qkv_weight.shape[1:], BF16),
            pltpu.VMEM(out_weight.shape[1:], BF16),
            pltpu.VMEM(out_weight.shape[1:], BF16),
            pltpu.VMEM((members, seqs, *memory.shape[3:]), BF16),
            pltpu.VMEM((members, seqs, *memory.shape[3:]), BF16),
            pltpu.VMEM(memory.shape[1:], BF16),
            pltpu.VMEM((seqs, heads_kv, group, blocks_local * block), F32),
            pltpu.VMEM((seqs, members, group, blocks_local * block), F32),
            pltpu.VMEM((members, *tile), F32),
            pltpu.VMEM((2, members, *tile), F32),
            pltpu.VMEM((2, *tile), F32),
            pltpu.VMEM((2, far, *tile), F32),
            pltpu.VMEM((2, members, seqs, group, head), BF16),
            pltpu.VMEM((2, members, *tile), F32),
            pltpu.VMEM((2, members, *tile), F32),
            pltpu.VMEM((2, *tile), F32),
            pltpu.VMEM((2, far, *tile), F32),
            pltpu.VMEM((seqs, group * head), F32),
            pltpu.VMEM((2, seqs, group * head), BF16),
            pltpu.VMEM((2, members, seqs, group * head), BF16),
            pltpu.VMEM((seqs, heads_total + width), BF16),
            pltpu.VMEM((seqs, heads_total + width), BF16),
            pltpu.SemaphoreType.DMA((8 + members,)),
            pltpu.SemaphoreType.DMA((2, 4)),
            pltpu.SemaphoreType.REGULAR,
            pltpu.SemaphoreType.DMA((4, members)),
            pltpu.SemaphoreType.DMA((12, slots)),
            pltpu.SemaphoreType.DMA((12, slots)),
        ],
        compiler_params=pltpu.CompilerParams(
            collective_id=0, has_side_effects=True, vmem_limit_bytes=VMEM_BYTES
        ),
        name="decode",
    )(lengths, hidden_in, norm_gain, selected, qkv_weight, out_weight, memory)
    return pl.pallas_call(
        functools.partial(hand_out, heads_total),
        out_shape=(
            jax.ShapeDtypeStruct((1, seqs, width), BF16),
            jax.ShapeDtypeStruct((1, seqs, heads_total), BF16),
        ),
        in_specs=[hbm],
        out_specs=(hbm, hbm),
        scratch_shapes=[pltpu.VMEM(result.shape, BF16), pltpu.SemaphoreType.DMA((3,))],
        name="hand_out",
    )(result)


def solution(mesh):
    z_size = mesh.shape["seq"] // RING_X
    finer = Mesh(
        mesh.devices.reshape(mesh.shape["groups"], RING_X, z_size, mesh.shape["section"]),
        ("groups", *SEQ, "section"),
    )
    in_specs = (
        P("groups", SEQ),
        P("section", SEQ),
        P("section", SEQ, None),
        P("section", None, SEQ),
        P("section", "groups", None, SEQ, None, None, None),
        P("groups"),
        P("groups", None, None),
    )
    out_specs = (P("section", "groups", SEQ), P("section", "groups", None))
    return jax.shard_map(body, mesh=finer, in_specs=in_specs, out_specs=out_specs, check_vma=False)
```
